32 devices in a mesh: dp: 8 (over y, x, core), mp: 4 (over z).
Axes of the slice: x: 2, y: 2, z: 4, core: 2. Of those that a mesh axis runs over, the one named last changes fastest.
Arguments:
- tokens: bfloat16 [8192, 2048], P(('dp', 'mp')), may hold values from -6 to 6
- cotangent: bfloat16 [8192, 2048], P(('dp', 'mp')), may hold values from -6 to 6
- ln1_gain: float32 [2048], replicated, may hold values from 0.5 to 1.5
- ln1_bias: float32 [2048], replicated, may hold values from -0.6 to 0.6
- w_qkv: bfloat16 [2048, 3, 2048], P(None, None, 'mp'), may hold values from -0.125 to 0.125
- w_out: bfloat16 [2048, 2048], P('mp'), may hold values from -1 to 1
- ln2_gain: float32 [2048], replicated, may hold values from 0.5 to 1.5
- ln2_bias: float32 [2048], replicated, may hold values from -0.6 to 0.6
- w_up: bfloat16 [2048, 8192], P(None, 'mp'), may hold values from -0.125 to 0.125
- w_down: bfloat16 [8192, 2048], P('mp'), may hold values from -0.0625 to 0.0625
- w_router: float32 [2048, 8], replicated, may hold values from -0.9 to 0.9
- seq_first: int32 [8], P('dp'), may hold values from 512 to 1024, as said below
- head_width: int32 [16], P('dp'), may hold values from 1 to 4
- ffn_width: int32 [16], P('dp'), may hold values from 1 to 4
Outputs:
- block_out: bfloat16 [8192, 2048], P(('dp', 'mp'))
- input_grad: bfloat16 [8192, 2048], P(('dp', 'mp'))
- ln1_gain_grad: float32 [2048], replicated
- ln1_bias_grad: float32 [2048], replicated
- qkv_weight_grad: float32 [2048, 3, 2048], P('dp', None, 'mp')
- out_weight_grad: float32 [2048, 2048], P('mp', 'dp')
- ln2_gain_grad: float32 [2048], replicated
- ln2_bias_grad: float32 [2048], replicated
- up_weight_grad: float32 [2048, 8192], P('dp', 'mp')
- down_weight_grad: float32 [8192, 2048], P('mp', 'dp')
- router_grad: float32 [2048, 8], replicated
The draws below stay inside these ranges and needn't reach their ends.
Inputs may be any that keep to these rules, and one draw needn't show every extreme that they name: Group g holds one sequence of 1024 rows where seq_first[g] = 1024, else two sequences of 512 rows; exactly half of the groups hold two. `head_width`: slot 2g + 1 has no rows where seq_first[g] = 1024. `ffn_width`: slot 2g + 1 has no rows where seq_first[g] = 1024.
All inputs are finite; a program needn't handle non-finite values.
Results may differ from the reference program's by a relative error of at most 0.025.
Values may be sent and summed in bfloat16 or wider, within the bound.
A program may use at most 192 MiB of HBM per device.

```python
import math
import jax
import jax.numpy as jnp
from jax import lax

D = 2048
HEADS = 16
HEAD_DIM = 128
FF = 8192
GTOK = 1024
GROUPS = 8
SLOTS = 16
TOKENS = 8192
N_MP = 4


def draw_seq_first(key, part):
    order = jax.random.permutation(key, GROUPS)
    return jnp.where(order < GROUPS // 2, GTOK // 2, GTOK).astype(jnp.int32)


def set_ends(array, stream_key, least, high):
    longest = array.shape.index(max(array.shape))
    spots = []
    for shift in (0, 1):
        where = [jax.random.randint(jax.random.fold_in(stream_key, axis), (), 0, length) for axis, length in enumerate(array.shape)]
        where[longest] = (where[longest] + shift) % array.shape[longest]
        spots.append(tuple(where))
    return array.at[spots[0]].set(least).at[spots[1]].set(high)


def spiked(array, own_key, source, target, parts, factor):
    owner, partner = [(jnp.arange(array.shape[dim]) // (array.shape[dim] // parts)).reshape([-1 if axis == dim else 1 for axis in range(array.ndim)]) for dim in (source, target)]
    chosen = jax.random.permutation(own_key, parts)[partner]
    strong = (owner == chosen) | (owner == (partner + parts // 2) % parts)
    return jnp.where(strong, factor * array, array)


def block_scale(stream_key, shape, cuts, least, high):
    loudness, own = 1.0, jax.random.fold_in(stream_key, 6)
    for dim, blocks in cuts:
        steps = jnp.exp(jax.random.uniform(jax.random.fold_in(own, dim), (blocks,), jnp.float32, least / len(cuts), high / len(cuts)))
        loudness = loudness * jnp.repeat(steps, shape[dim] // blocks).reshape([-1 if axis == dim else 1 for axis in range(len(shape))])
    return loudness


def gaussian(stream_key, dims, width, reach, cuts=(), kind=jnp.bfloat16):
    factor_of = block_scale(stream_key, dims, cuts, -0.22, 0.18) if cuts else 1.0
    array = jax.random.normal(stream_key, dims, jnp.float32) * width * factor_of
    return jnp.minimum(jnp.maximum(array, -reach), reach).astype(kind)


def bell_draw_with(key, extent, scale, bound, shards, heavy, kind=jnp.bfloat16):
    drawn = scale * jax.random.normal(key, extent, jnp.float32)
    if shards:
        drawn = drawn * block_scale(key, extent, shards, -0.22, 0.18)
    return jnp.clip(spiked(drawn, jax.random.fold_in(key, 3), *heavy), -bound, bound).astype(kind)


def setup_inputs(seed: int = 0) -> dict:
    arg_keys = jax.random.split(jax.random.key(seed), 15)
    return {
        "tokens": gaussian(arg_keys[0], (TOKENS, D), 1.0, 6.0, ((0, 32),)),
        "cotangent": bell_draw_with(arg_keys[1], (TOKENS, D), 1.0, 6.0, ((0, 32),), (0, 1, 32, 2.75)),
        "ln1_gain": jnp.clip(1.0 + 0.1 * jax.random.normal(arg_keys[2], (D,), jnp.float32), 0.5, 1.5),
        "ln1_bias": gaussian(arg_keys[3], (D,), 0.1, 0.6, (), jnp.float32),
        "w_qkv": gaussian(arg_keys[4], (D, 3, D), D ** -0.5, 0.125, ((2, 4),)),
        "w_out": gaussian(arg_keys[5], (D, D), (D // 64) ** -0.5, 1.0, ((0, 4),)),
        "ln2_gain": jnp.clip(1.0 + 0.1 * jax.random.normal(arg_keys[6], (D,), jnp.float32), 0.5, 1.5),
        "ln2_bias": gaussian(arg_keys[7], (D,), 0.1, 0.6, (), jnp.float32),
        "w_up": gaussian(arg_keys[8], (D, FF), D ** -0.5, 0.125, ((1, 4),)),
        "w_down": gaussian(arg_keys[9], (FF, D), FF ** -0.5, 0.0625, ((0, 4),)),
        "w_router": gaussian(arg_keys[10], (D, 2 * N_MP), 0.15, 0.9, (), jnp.float32),
        "seq_first": draw_seq_first(jax.random.fold_in(arg_keys[14], 71), 0),
        "head_width": set_ends(jax.random.randint(arg_keys[12], (SLOTS,), 1, N_MP + 1), jax.random.fold_in(arg_keys[12], 1), 1, N_MP).astype(jnp.int32),
        "ffn_width": set_ends(jax.random.randint(arg_keys[13], (SLOTS,), 1, N_MP + 1), jax.random.fold_in(arg_keys[13], 1), 1, N_MP).astype(jnp.int32),
    }


@jax.custom_vjp
def low(v):
    return lax.optimization_barrier(v.astype(jnp.bfloat16)).astype(jnp.float32)

@jax.custom_vjp
def low_back(v):
    return v

def low_keep(v):
    return (low(v), None)

def low_pass(kept, grad):
    return (grad,)

def back_keep(v):
    return (v, None)

def back_low(kept, grad):
    return (low(grad),)
low.defvjp(low_keep, low_pass)
low_back.defvjp(back_keep, back_low)
epsilon = 1e-05
masked_score = -1000000000.0

def matmul(left, right):
    return jnp.dot(left, right, precision=lax.Precision.HIGHEST, preferred_element_type=jnp.float32)

def layer_norm(values, gain_vec, bias_vec):
    center = values - lax.optimization_barrier(jnp.mean(values, -1, keepdims=True))
    inv_std = lax.rsqrt(lax.optimization_barrier(jnp.mean(center * center, -1, keepdims=True)) + epsilon)
    return center * inv_std * gain_vec + bias_vec

def rotary_tables(positions, full_width):
    half_width = full_width // 2
    frequency = jnp.exp(jnp.arange(half_width, dtype=jnp.float32) * (-2.0 * math.log(10000.0) / full_width))
    angles = positions[:, None] * frequency[None, :]
    cosine = jnp.cos(angles)
    sine_rows = jnp.sin(angles)
    return (jnp.concatenate([cosine, cosine], -1), jnp.concatenate([sine_rows, sine_rows], -1))

def rotate(values, cosine, sine_rows):
    half_width = values.shape[-1] // 2
    turned = jnp.concatenate([-values[..., half_width:], values[..., :half_width]], -1)
    return values * cosine + turned * sine_rows

def group_layer(params, group_rows, split_at, head_pick, ffn_pick):
    ln1_gain, ln1_bias, w_qkv, w_out, ln2_gain, ln2_bias, w_up, w_down, w_router = params
    row_ids = jnp.arange(GTOK, dtype=jnp.int32)
    row_slot = (row_ids >= split_at).astype(jnp.int32)
    positions = (row_ids - row_slot * split_at).astype(jnp.float32)
    slot_hot = (row_slot[None, :] == jnp.arange(2, dtype=jnp.int32)[:, None]).astype(jnp.float32)
    counts = jnp.maximum(lax.optimization_barrier(jnp.sum(slot_hot, 1)), 1.0)
    h_one = low(layer_norm(group_rows, ln1_gain, ln1_bias))
    slot_means = matmul(slot_hot, h_one) / counts[:, None]
    logits = matmul(slot_means, w_router)
    levels = jnp.arange(N_MP, dtype=jnp.int32)
    prob_head = jax.nn.softmax(logits[:, :N_MP], -1)
    prob_ffn = jax.nn.softmax(logits[:, N_MP:], -1)
    scale_head = N_MP * lax.optimization_barrier(jnp.sum(prob_head * (levels[None, :] == head_pick[:, None] - 1), 1))
    scale_ffn = N_MP * lax.optimization_barrier(jnp.sum(prob_ffn * (levels[None, :] == ffn_pick[:, None] - 1), 1))
    qkv_rows = low_back(matmul(h_one, w_qkv.reshape(D, 3 * D))).reshape(GTOK, 3, HEADS, HEAD_DIM)
    cosine, sine_rows = rotary_tables(positions, HEAD_DIM)
    query = low(rotate(qkv_rows[:, 0], cosine[:, None, :], sine_rows[:, None, :]))
    key_rows = low(rotate(qkv_rows[:, 1], cosine[:, None, :], sine_rows[:, None, :]))
    value = low(qkv_rows[:, 2])
    scores = jnp.einsum('thd,shd->hts', query, key_rows, precision=lax.Precision.HIGHEST) * (1.0 / math.sqrt(HEAD_DIM))
    scores = low_back(scores)
    allowed = (row_slot[:, None] == row_slot[None, :]) & (row_ids[None, :] <= row_ids[:, None])
    scores = jnp.where(allowed[None], scores, masked_score)
    prob_rows = low(jax.nn.softmax(scores, -1))
    heads_out = jnp.einsum('hts,shd->thd', prob_rows, value, precision=lax.Precision.HIGHEST)
    head_group = jnp.arange(HEADS, dtype=jnp.int32) // (HEADS // N_MP)
    head_on = (head_group[None, :] < head_pick[row_slot][:, None]).astype(jnp.float32)
    mixed = low_back(low(heads_out * head_on[:, :, None])).reshape(GTOK, D)
    attn_branch = low_back(matmul(mixed, w_out))
    mid = group_rows + scale_head[row_slot][:, None] * attn_branch
    h_two = low(layer_norm(mid, ln2_gain, ln2_bias))
    up_proj = low_back(matmul(h_two, w_up))
    col_group = jnp.arange(FF, dtype=jnp.int32) // (FF // N_MP)
    ffn_on = (col_group[None, :] < ffn_pick[row_slot][:, None]).astype(jnp.float32)
    hidden = low_back(low(jnp.square(jnp.maximum(up_proj, 0.0)) * ffn_on))
    ffn_branch = low_back(matmul(hidden, w_down))
    return mid + scale_ffn[row_slot][:, None] * ffn_branch

def forward(tokens, ln1_gain, ln1_bias, w_qkv, w_out, ln2_gain, ln2_bias, w_up, w_down, w_router, seq_first, head_width, ffn_width):
    params = (ln1_gain, ln1_bias, w_qkv, w_out, ln2_gain, ln2_bias, w_up, w_down, w_router)

    def one_group(group_item):
        return group_layer(params, group_item[0], group_item[1], group_item[2], group_item[3])
    layer_out = lax.map(jax.checkpoint(one_group), (tokens.reshape(GROUPS, GTOK, D), seq_first, head_width.reshape(GROUPS, 2), ffn_width.reshape(GROUPS, 2)))
    return layer_out.reshape(TOKENS, D)

def reference(tokens, cotangent, ln1_gain, ln1_bias, w_qkv, w_out, ln2_gain, ln2_bias, w_up, w_down, w_router, seq_first, head_width, ffn_width):
    floats = (tokens.astype(jnp.float32), ln1_gain, ln1_bias, w_qkv.astype(jnp.float32), w_out.astype(jnp.float32), ln2_gain, ln2_bias, w_up.astype(jnp.float32), w_down.astype(jnp.float32), w_router)

    def run_layer(*values):
        return forward(*values, seq_first, head_width, ffn_width)
    layer_out, pullback = jax.vjp(run_layer, *floats)
    grads = pullback(cotangent.astype(jnp.float32))
    return (layer_out.astype(jnp.bfloat16), grads[0].astype(jnp.bfloat16), grads[1], grads[2], grads[3], grads[4], grads[5], grads[6], grads[7], grads[8], grads[9])
```

```python
import math

import jax
import jax.numpy as jnp
from jax import lax
from jax.sharding import PartitionSpec as P

D = 2048
HEAD_DIM = 128
CHUNKS = 2


epsilon = 1e-05
masked_score = -1000000000.0


def norm_rows(values, gain_vec, bias_vec):
    center = values - jnp.mean(values, -1, keepdims=True)
    inv_std = lax.rsqrt(jnp.mean(center * center, -1, keepdims=True) + epsilon)
    unit_rows = center * inv_std
    return (unit_rows * gain_vec + bias_vec, unit_rows, inv_std)


def norm_back(grad_rows, unit_rows, inv_std, gain_vec):
    scaled = grad_rows * gain_vec
    inner = (
        scaled
        - jnp.mean(scaled, -1, keepdims=True)
        - unit_rows * jnp.mean(scaled * unit_rows, -1, keepdims=True)
    )
    return (inner * inv_std, jnp.sum(grad_rows * unit_rows, 0), jnp.sum(grad_rows, 0))


def rotary_tables(positions, full_width):
    half_width = full_width // 2
    frequency = jnp.exp(
        jnp.arange(half_width, dtype=jnp.float32) * (-2.0 * math.log(10000.0) / full_width)
    )
    angles = positions[:, None] * frequency[None, :]
    cosine = jnp.cos(angles)
    sine_rows = jnp.sin(angles)
    return (jnp.concatenate([cosine, cosine], -1), jnp.concatenate([sine_rows, sine_rows], -1))


def rotate(values, cosine, sine_rows):
    half_width = values.shape[-1] // 2
    turned = jnp.concatenate([-values[..., half_width:], values[..., :half_width]], -1)
    return values * cosine + turned * sine_rows


def rotate_back(grad_rows, cosine, sine_rows):
    half_width = grad_rows.shape[-1] // 2
    moved = grad_rows * sine_rows
    turned = jnp.concatenate([moved[..., half_width:], -moved[..., :half_width]], -1)
    return grad_rows * cosine + turned


def gather_rows(block):
    shard_count = lax.axis_size("mp")
    parts = [block]
    for shift in range(1, shard_count):
        pairs = [(owner, (owner + shift) % shard_count) for owner in range(shard_count)]
        parts.append(lax.ppermute(block, "mp", pairs))
    return jnp.concatenate(parts, 0)


def scatter_rows(partial):
    shard_count = lax.axis_size("mp")
    rows = partial.shape[0] // shard_count
    total = partial[:rows].astype(jnp.float32)
    for shift in range(1, shard_count):
        pairs = [(holder, (holder - shift) % shard_count) for holder in range(shard_count)]
        sent = partial[shift * rows : (shift + 1) * rows]
        total = total + lax.ppermute(sent, "mp", pairs).astype(jnp.float32)
    return total


def swap_bit(values, axis_name, bit):
    size = lax.axis_size(axis_name)
    return lax.ppermute(values, axis_name, [(one, one ^ (1 << bit)) for one in range(size)])


def scatter_groups(values, flip):
    size = lax.axis_size("dp")
    bits = size.bit_length() - 1
    mine = lax.axis_index("dp")
    order = list(range(bits))
    if flip:
        order = order[:1] + order[1:][::-1]
    left = list(range(bits))[::-1]
    held = values.reshape((2,) * bits + (values.shape[0] // size,) + values.shape[1:])
    for step, bit in enumerate(order):
        axis = left.index(bit)
        own_bit = (mine >> bit) & 1
        sent = lax.dynamic_index_in_dim(held, 1 - own_bit, axis, keepdims=False)
        kept = lax.dynamic_index_in_dim(held, own_bit, axis, keepdims=False)
        held = kept.astype(jnp.float32) + swap_bit(sent, "dp", bit).astype(jnp.float32)
        if step < bits - 1:
            held = held.astype(jnp.bfloat16)
        left.remove(bit)
    return held


def sum_over(values, axis_name):
    for bit in range(lax.axis_size(axis_name).bit_length() - 1):
        values = values + swap_bit(values, axis_name, bit)
    return values


def sum_all(values):
    return sum_over(sum_over(values, "dp"), "mp")


def local(
    tokens,
    cotangent,
    ln1_gain,
    ln1_bias,
    w_qkv,
    w_out,
    ln2_gain,
    ln2_bias,
    w_up,
    w_down,
    w_router,
    seq_first,
    head_width,
    ffn_width,
):
    shard_count = lax.axis_size("mp")
    mp_index = lax.axis_index("mp")
    tok_dev = tokens.shape[0]
    group_rows = tok_dev * shard_count
    part_rows = tok_dev // CHUNKS
    chunk_rows = group_rows // CHUNKS
    local_dim = w_qkv.shape[2]
    heads_here = local_dim // HEAD_DIM
    split_at = seq_first[0]

    def cut(values):
        return [values[c * part_rows : (c + 1) * part_rows] for c in range(CHUNKS)]

    def cut_all(values):
        return [values[c * chunk_rows : (c + 1) * chunk_rows] for c in range(CHUNKS)]

    own_rows = mp_index * tok_dev + jnp.arange(tok_dev, dtype=jnp.int32)
    owners = (mp_index - jnp.arange(shard_count, dtype=jnp.int32)) % shard_count
    row_ids = (
        owners[None, :, None] * tok_dev
        + jnp.arange(CHUNKS, dtype=jnp.int32)[:, None, None] * part_rows
        + jnp.arange(part_rows, dtype=jnp.int32)[None, None, :]
    ).reshape(group_rows)
    row_slot = (row_ids >= split_at).astype(jnp.int32)
    positions = (row_ids - row_slot * split_at).astype(jnp.float32)
    slot_hot = (row_slot[None, :] == jnp.arange(2, dtype=jnp.int32)[:, None]).astype(jnp.float32)
    counts = jnp.maximum(jnp.sum(slot_hot, 1), 1.0)
    own_slot = (own_rows >= split_at).astype(jnp.int32)
    own_hot = (own_slot[:, None] == jnp.arange(2, dtype=jnp.int32)[None, :]).astype(jnp.float32)
    head_on = (mp_index < jnp.where(row_slot == 1, head_width[1], head_width[0])).astype(
        jnp.float32
    )
    ffn_on = (mp_index < jnp.where(row_slot == 1, ffn_width[1], ffn_width[0])).astype(jnp.float32)
    x_rows = tokens.astype(jnp.float32)
    normed1, unit1, inv_std1 = norm_rows(x_rows, ln1_gain, ln1_bias)
    h_one = normed1.astype(jnp.bfloat16)
    h_one_parts = [gather_rows(part) for part in cut(h_one)]
    h_one_parts, late_cotangent = lax.optimization_barrier((h_one_parts, cotangent))
    cotangent_parts = [gather_rows(part) for part in cut(late_cotangent)]
    h_one_all = jnp.concatenate(h_one_parts, 0)
    slot_means = (
        jnp.dot(slot_hot.astype(jnp.bfloat16), h_one_all, preferred_element_type=jnp.float32)
        / counts[:, None]
    )
    logits = jnp.dot(slot_means, w_router, precision=lax.Precision.HIGHEST)
    levels = jnp.arange(shard_count, dtype=jnp.int32)
    pick_head = (levels[None, :] == head_width[:, None] - 1).astype(jnp.float32)
    pick_ffn = (levels[None, :] == ffn_width[:, None] - 1).astype(jnp.float32)
    prob_head = jax.nn.softmax(logits[:, :shard_count], -1)
    prob_ffn = jax.nn.softmax(logits[:, shard_count:], -1)
    scale_head = shard_count * jnp.sum(prob_head * pick_head, 1)
    scale_ffn = shard_count * jnp.sum(prob_ffn * pick_ffn, 1)
    own_scale_head = jnp.where(own_slot == 1, scale_head[1], scale_head[0])[:, None]
    own_scale_ffn = jnp.where(own_slot == 1, scale_ffn[1], scale_ffn[0])[:, None]
    row_scale_ffn = jnp.where(row_slot == 1, scale_ffn[1], scale_ffn[0])[:, None]
    w_qkv_flat = w_qkv.reshape(D, 3 * local_dim)
    qkv_rows = jnp.dot(h_one_all, w_qkv_flat, preferred_element_type=jnp.float32).reshape(
        group_rows, 3, heads_here, HEAD_DIM
    )
    cosine, sine_rows = rotary_tables(positions, HEAD_DIM)
    cosine_b = cosine[:, None, :]
    sine_b = sine_rows[:, None, :]
    query = rotate(qkv_rows[:, 0], cosine_b, sine_b).astype(jnp.bfloat16)
    key_rows = rotate(qkv_rows[:, 1], cosine_b, sine_b).astype(jnp.bfloat16)
    value = qkv_rows[:, 2].astype(jnp.bfloat16)
    inv_root = 1.0 / math.sqrt(HEAD_DIM)
    query_parts = cut_all(query)
    slot_parts = cut_all(row_slot)
    id_parts = cut_all(row_ids)
    head_on_parts = cut_all(head_on)
    ffn_on_parts = cut_all(ffn_on)
    scale_ffn_parts = cut_all(row_scale_ffn)

    def scores_block(c):
        raw_scores = (
            jnp.einsum("thd,shd->hts", query_parts[c], key_rows, preferred_element_type=jnp.float32)
            * inv_root
        )
        allowed = (slot_parts[c][:, None] == row_slot[None, :]) & (
            row_ids[None, :] <= id_parts[c][:, None]
        )
        return jnp.where(allowed[None], raw_scores, masked_score)

    lse_list = []
    mixed_parts = []
    attn_branch_parts = []
    for c in range(CHUNKS):
        block_scores = scores_block(c)
        row_top = jnp.max(block_scores, -1, keepdims=True)
        exp_scores = jnp.exp(block_scores - row_top)
        row_total = jnp.sum(exp_scores, -1, keepdims=True)
        prob_rows = exp_scores / row_total
        lse_list.append(row_top + jnp.log(row_total))
        heads_out = jnp.einsum(
            "hts,shd->thd",
            prob_rows.astype(jnp.bfloat16),
            value,
            preferred_element_type=jnp.float32,
        )
        mixed = (
            (heads_out * head_on_parts[c][:, None, None])
            .astype(jnp.bfloat16)
            .reshape(chunk_rows, local_dim)
        )
        mixed_parts.append(mixed)
        attn_branch_parts.append(
            scatter_rows(
                jnp.dot(mixed, w_out, preferred_element_type=jnp.float32).astype(jnp.bfloat16)
            )
        )
    x_parts = cut(x_rows)
    scale_head_own = cut(own_scale_head)
    scale_ffn_own = cut(own_scale_ffn)
    grad_out = cotangent.astype(jnp.float32)
    grad_out_parts = cut(grad_out)
    own_hot_parts = cut(own_hot)
    mid_parts = []
    norm2_parts = []
    h_two_parts = []
    for c in range(CHUNKS):
        mid_rows = x_parts[c] + scale_head_own[c] * attn_branch_parts[c]
        normed2, unit2, inv_std2 = norm_rows(mid_rows, ln2_gain, ln2_bias)
        mid_parts.append(mid_rows)
        norm2_parts.append((unit2, inv_std2))
        h_two_parts.append(gather_rows(normed2.astype(jnp.bfloat16)))
    hidden_parts = []
    ffn_grad_parts = []
    grad_up_parts = []
    normed2_grad_parts = []
    for c in range(CHUNKS):
        ffn_grad = (scale_ffn_parts[c] * cotangent_parts[c].astype(jnp.float32)).astype(
            jnp.bfloat16
        )
        hidden_grad = jnp.dot(ffn_grad, w_down.T, preferred_element_type=jnp.float32).astype(
            jnp.bfloat16
        )
        up_proj = jnp.dot(h_two_parts[c], w_up, preferred_element_type=jnp.float32)
        relu_rows = jnp.maximum(up_proj, 0.0)
        on_rows = ffn_on_parts[c][:, None]
        hidden_parts.append((relu_rows * relu_rows * on_rows).astype(jnp.bfloat16))
        grad_up = (hidden_grad.astype(jnp.float32) * (2.0 * relu_rows * on_rows)).astype(
            jnp.bfloat16
        )
        ffn_grad_parts.append(ffn_grad)
        grad_up_parts.append(grad_up)
        normed2_grad_parts.append(
            scatter_rows(
                jnp.dot(grad_up, w_up.T, preferred_element_type=jnp.float32).astype(jnp.bfloat16)
            )
        )
    mid_grad_parts = []
    attn_grad_sent = []
    gain2_grad = 0.0
    bias2_grad = 0.0
    part_head = 0.0
    for c in range(CHUNKS):
        unit2, inv_std2 = norm2_parts[c]
        back_two, gain_part, bias_part = norm_back(
            normed2_grad_parts[c], unit2, inv_std2, ln2_gain
        )
        gain2_grad = gain2_grad + gain_part
        bias2_grad = bias2_grad + bias_part
        mid_grad = grad_out_parts[c] + back_two
        part_head = part_head + jnp.sum(
            own_hot_parts[c] * jnp.sum(mid_grad * attn_branch_parts[c], 1, keepdims=True), 0
        )
        mid_grad_parts.append(mid_grad)
        attn_grad_sent.append((scale_head_own[c] * mid_grad).astype(jnp.bfloat16))
    attn_grad_parts = [gather_rows(part) for part in attn_grad_sent]
    hidden_parts, ffn_grad_parts, grad_up_parts, h_two_parts, _ = lax.optimization_barrier(
        (hidden_parts, ffn_grad_parts, grad_up_parts, h_two_parts, attn_grad_sent)
    )
    hidden_all = jnp.concatenate(hidden_parts, 0)
    ffn_grad_all = jnp.concatenate(ffn_grad_parts, 0)
    grad_up_all = jnp.concatenate(grad_up_parts, 0)
    h_two_all = jnp.concatenate(h_two_parts, 0)
    down_grad = scatter_groups(
        jnp.dot(ffn_grad_all.T, hidden_all, preferred_element_type=jnp.float32).astype(
            jnp.bfloat16
        ),
        False,
    )
    up_grad = scatter_groups(
        jnp.dot(h_two_all.T, grad_up_all, preferred_element_type=jnp.float32).astype(jnp.bfloat16),
        True,
    )
    ffn_full = jnp.dot(hidden_all, w_down, preferred_element_type=jnp.float32).astype(jnp.bfloat16)
    ffn_branch = jnp.concatenate([scatter_rows(part) for part in cut_all(ffn_full)], 0)
    mid_all = jnp.concatenate(mid_parts, 0)
    block_out = (mid_all + own_scale_ffn * ffn_branch).astype(jnp.bfloat16)
    part_ffn = jnp.sum(own_hot * jnp.sum(grad_out * ffn_branch, 1, keepdims=True), 0)
    scale_grads = sum_over(jnp.stack([part_head, part_ffn]), "mp")
    logit_head_grad = (scale_grads[0] * scale_head)[:, None] * (pick_head - prob_head)
    logit_ffn_grad = (scale_grads[1] * scale_ffn)[:, None] * (pick_ffn - prob_ffn)
    logit_grad = jnp.concatenate([logit_head_grad, logit_ffn_grad], 1)
    router_part = jnp.dot(logit_grad.T, slot_means, precision=lax.Precision.HIGHEST) / shard_count
    early_sums = sum_all(
        jnp.concatenate([gain2_grad[None], bias2_grad[None], router_part], 0)
    )
    mean_grad = jnp.dot(logit_grad, w_router.T, precision=lax.Precision.HIGHEST) / counts[:, None]
    key_grad = 0.0
    value_grad = 0.0
    query_grads = []
    for c in range(CHUNKS):
        grad_blk = (
            jnp.dot(attn_grad_parts[c], w_out.T, preferred_element_type=jnp.float32)
            .astype(jnp.bfloat16)
            .reshape(chunk_rows, heads_here, HEAD_DIM)
        ) * head_on_parts[c].astype(jnp.bfloat16)[:, None, None]
        block_scores = scores_block(c)
        prob_rows = jnp.exp(block_scores - lse_list[c])
        prob_grad = jnp.einsum("thd,shd->hts", grad_blk, value, preferred_element_type=jnp.float32)
        delta = jnp.sum(prob_rows * prob_grad, -1, keepdims=True)
        score_grad = (prob_rows * (prob_grad - delta)).astype(jnp.bfloat16)
        query_grads.append(
            jnp.einsum("hts,shd->thd", score_grad, key_rows, preferred_element_type=jnp.float32)
            * inv_root
        )
        key_grad = (
            key_grad
            + jnp.einsum(
                "hts,thd->shd", score_grad, query_parts[c], preferred_element_type=jnp.float32
            )
            * inv_root
        )
        value_grad = value_grad + jnp.einsum(
            "hts,thd->shd",
            prob_rows.astype(jnp.bfloat16),
            grad_blk,
            preferred_element_type=jnp.float32,
        )
    query_grad = jnp.concatenate(query_grads, 0)
    qkv_grad = jnp.stack(
        [
            rotate_back(query_grad, cosine_b, sine_b),
            rotate_back(key_grad, cosine_b, sine_b),
            value_grad,
        ],
        1,
    )
    qkv_grad = qkv_grad.astype(jnp.bfloat16).reshape(group_rows, 3 * local_dim)
    normed1_sent = [
        jnp.dot(part, w_qkv_flat.T, preferred_element_type=jnp.float32).astype(jnp.bfloat16)
        for part in cut_all(qkv_grad)
    ]
    normed1_grad = jnp.concatenate([scatter_rows(part) for part in normed1_sent], 0)
    qkv_late, _ = lax.optimization_barrier((qkv_grad, normed1_sent))
    qkv_weight_grad = scatter_groups(
        jnp.dot(h_one_all.T, qkv_late, preferred_element_type=jnp.float32).astype(jnp.bfloat16),
        False,
    ).reshape(-1, 3, local_dim)
    attn_grad_all = jnp.concatenate(attn_grad_parts, 0)
    attn_mixed = jnp.concatenate(mixed_parts, 0)
    out_grad = scatter_groups(
        jnp.dot(attn_grad_all.T, attn_mixed, preferred_element_type=jnp.float32).astype(
            jnp.bfloat16
        ),
        True,
    )
    normed1_grad = normed1_grad + jnp.dot(own_hot, mean_grad, precision=lax.Precision.HIGHEST)
    back_one, gain1_grad, bias1_grad = norm_back(normed1_grad, unit1, inv_std1, ln1_gain)
    input_grad = (jnp.concatenate(mid_grad_parts, 0) + back_one).astype(jnp.bfloat16)
    late_sums = sum_all(jnp.stack([gain1_grad, bias1_grad]))
    return (
        block_out,
        input_grad,
        late_sums[0],
        late_sums[1],
        qkv_weight_grad,
        out_grad.T,
        early_sums[0],
        early_sums[1],
        up_grad,
        down_grad.T,
        early_sums[2:].T,
    )


def solution(mesh):
    placed = (
        P(("dp", "mp"), None),
        P(("dp", "mp"), None),
        P(),
        P(),
        P(None, None, "mp"),
        P("mp", None),
        P(),
        P(),
        P(None, "mp"),
        P("mp", None),
        P(),
        P("dp"),
        P("dp"),
        P("dp"),
    )
    return jax.shard_map(
        local,
        mesh=mesh,
        in_specs=placed,
        out_specs=(
            P(("dp", "mp"), None),
            P(("dp", "mp"), None),
            P(),
            P(),
            P("dp", None, "mp"),
            P("mp", "dp"),
            P(),
            P(),
            P("dp", "mp"),
            P("mp", "dp"),
            P(),
        ),
        check_vma=False,
    )
```

```python
import math

import jax
import jax.numpy as jnp
from jax import lax
from jax.sharding import PartitionSpec as P

D = 2048
HEAD_DIM = 128
CHUNKS = 2


epsilon = 1e-05
masked_score = -1000000000.0


def norm_rows(values, gain_vec, bias_vec):
    center = values - jnp.mean(values, -1, keepdims=True)
    inv_std = lax.rsqrt(jnp.mean(center * center, -1, keepdims=True) + epsilon)
    unit_rows = center * inv_std
    return (unit_rows * gain_vec + bias_vec, unit_rows, inv_std)


def norm_back(grad_rows, unit_rows, inv_std, gain_vec):
    scaled = grad_rows * gain_vec
    inner = (
        scaled
        - jnp.mean(scaled, -1, keepdims=True)
        - unit_rows * jnp.mean(scaled * unit_rows, -1, keepdims=True)
    )
    return (inner * inv_std, jnp.sum(grad_rows * unit_rows, 0), jnp.sum(grad_rows, 0))


def rotary_tables(positions, full_width):
    half_width = full_width // 2
    frequency = jnp.exp(
        jnp.arange(half_width, dtype=jnp.float32) * (-2.0 * math.log(10000.0) / full_width)
    )
    angles = positions[:, None] * frequency[None, :]
    cosine = jnp.cos(angles)
    sine_rows = jnp.sin(angles)
    return (jnp.concatenate([cosine, cosine], -1), jnp.concatenate([sine_rows, sine_rows], -1))


def rotate(values, cosine, sine_rows):
    half_width = values.shape[-1] // 2
    turned = jnp.concatenate([-values[..., half_width:], values[..., :half_width]], -1)
    return values * cosine + turned * sine_rows


def rotate_back(grad_rows, cosine, sine_rows):
    half_width = grad_rows.shape[-1] // 2
    moved = grad_rows * sine_rows
    turned = jnp.concatenate([moved[..., half_width:], -moved[..., :half_width]], -1)
    return grad_rows * cosine + turned


def gather_rows(block):
    shard_count = lax.axis_size("mp")
    parts = [block]
    for shift in range(1, shard_count):
        pairs = [(owner, (owner + shift) % shard_count) for owner in range(shard_count)]
        parts.append(lax.ppermute(block, "mp", pairs))
    return jnp.concatenate(parts, 0)


def send_rows(partial):
    shard_count = lax.axis_size("mp")
    rows = partial.shape[0] // shard_count
    parts = [partial[:rows]]
    for shift in range(1, shard_count):
        pairs = [(holder, (holder - shift) % shard_count) for holder in range(shard_count)]
        parts.append(lax.ppermute(partial[shift * rows : (shift + 1) * rows], "mp", pairs))
    return parts


def sum_parts(parts):
    total = parts[0].astype(jnp.float32)
    for part in parts[1:]:
        total = total + part.astype(jnp.float32)
    return total


def scatter_rows(partial):
    return sum_parts(send_rows(partial))


def swap_bit(values, axis_name, bit):
    size = lax.axis_size(axis_name)
    return lax.ppermute(values, axis_name, [(one, one ^ (1 << bit)) for one in range(size)])


def scatter_groups(values, dim):
    return lax.psum_scatter(values, "dp", scatter_dimension=dim, tiled=True)


def sum_over(values, axis_name):
    for bit in range(lax.axis_size(axis_name).bit_length() - 1):
        values = values + swap_bit(values, axis_name, bit)
    return values


def sum_all(values):
    return sum_over(sum_over(values, "mp"), "dp")


def local(
    tokens,
    cotangent,
    ln1_gain,
    ln1_bias,
    w_qkv,
    w_out,
    ln2_gain,
    ln2_bias,
    w_up,
    w_down,
    w_router,
    seq_first,
    head_width,
    ffn_width,
):
    shard_count = lax.axis_size("mp")
    mp_index = lax.axis_index("mp")
    tok_dev = tokens.shape[0]
    group_rows = tok_dev * shard_count
    part_rows = tok_dev // CHUNKS
    chunk_rows = group_rows // CHUNKS
    local_dim = w_qkv.shape[2]
    heads_here = local_dim // HEAD_DIM
    split_at = seq_first[0]

    def cut(values):
        return [values[c * part_rows : (c + 1) * part_rows] for c in range(CHUNKS)]

    def cut_all(values):
        return [values[c * chunk_rows : (c + 1) * chunk_rows] for c in range(CHUNKS)]

    own_rows = mp_index * tok_dev + jnp.arange(tok_dev, dtype=jnp.int32)
    owners = (mp_index - jnp.arange(shard_count, dtype=jnp.int32)) % shard_count
    row_ids = (
        owners[None, :, None] * tok_dev
        + jnp.arange(CHUNKS, dtype=jnp.int32)[:, None, None] * part_rows
        + jnp.arange(part_rows, dtype=jnp.int32)[None, None, :]
    ).reshape(group_rows)
    row_slot = (row_ids >= split_at).astype(jnp.int32)
    positions = (row_ids - row_slot * split_at).astype(jnp.float32)
    slot_hot = (row_slot[None, :] == jnp.arange(2, dtype=jnp.int32)[:, None]).astype(jnp.float32)
    counts = jnp.maximum(jnp.sum(slot_hot, 1), 1.0)
    own_slot = (own_rows >= split_at).astype(jnp.int32)
    own_hot = (own_slot[:, None] == jnp.arange(2, dtype=jnp.int32)[None, :]).astype(jnp.float32)
    head_on = (mp_index < jnp.where(row_slot == 1, head_width[1], head_width[0])).astype(
        jnp.float32
    )
    ffn_on = (mp_index < jnp.where(row_slot == 1, ffn_width[1], ffn_width[0])).astype(jnp.float32)
    x_rows = tokens.astype(jnp.float32)
    normed1, unit1, inv_std1 = norm_rows(x_rows, ln1_gain, ln1_bias)
    h_one = normed1.astype(jnp.bfloat16)
    h_one_parts = [gather_rows(part) for part in cut(h_one)]
    h_one_parts, late_cotangent = lax.optimization_barrier((h_one_parts, cotangent))
    cotangent_parts = [gather_rows(part) for part in cut(late_cotangent)]
    h_one_all = jnp.concatenate(h_one_parts, 0)
    slot_means = (
        jnp.dot(slot_hot.astype(jnp.bfloat16), h_one_all, preferred_element_type=jnp.float32)
        / counts[:, None]
    )
    logits = jnp.dot(slot_means, w_router, precision=lax.Precision.HIGHEST)
    levels = jnp.arange(shard_count, dtype=jnp.int32)
    pick_head = (levels[None, :] == head_width[:, None] - 1).astype(jnp.float32)
    pick_ffn = (levels[None, :] == ffn_width[:, None] - 1).astype(jnp.float32)
    prob_head = jax.nn.softmax(logits[:, :shard_count], -1)
    prob_ffn = jax.nn.softmax(logits[:, shard_count:], -1)
    scale_head = shard_count * jnp.sum(prob_head * pick_head, 1)
    scale_ffn = shard_count * jnp.sum(prob_ffn * pick_ffn, 1)
    own_scale_head = jnp.where(own_slot == 1, scale_head[1], scale_head[0])[:, None]
    own_scale_ffn = jnp.where(own_slot == 1, scale_ffn[1], scale_ffn[0])[:, None]
    row_scale_ffn = jnp.where(row_slot == 1, scale_ffn[1], scale_ffn[0])[:, None]
    w_qkv_flat = w_qkv.reshape(D, 3 * local_dim)
    qkv_rows = jnp.dot(h_one_all, w_qkv_flat, preferred_element_type=jnp.float32).reshape(
        group_rows, 3, heads_here, HEAD_DIM
    )
    cosine, sine_rows = rotary_tables(positions, HEAD_DIM)
    cosine_b = cosine[:, None, :]
    sine_b = sine_rows[:, None, :]
    query = rotate(qkv_rows[:, 0], cosine_b, sine_b).astype(jnp.bfloat16)
    key_rows = rotate(qkv_rows[:, 1], cosine_b, sine_b).astype(jnp.bfloat16)
    value = qkv_rows[:, 2].astype(jnp.bfloat16)
    inv_root = 1.0 / math.sqrt(HEAD_DIM)
    query_parts = cut_all(query)
    slot_parts = cut_all(row_slot)
    id_parts = cut_all(row_ids)
    head_on_parts = cut_all(head_on)
    ffn_on_parts = cut_all(ffn_on)
    scale_ffn_parts = cut_all(row_scale_ffn)

    def scores_block(c):
        raw_scores = (
            jnp.einsum("thd,shd->hts", query_parts[c], key_rows, preferred_element_type=jnp.float32)
            * inv_root
        )
        allowed = (slot_parts[c][:, None] == row_slot[None, :]) & (
            row_ids[None, :] <= id_parts[c][:, None]
        )
        return jnp.where(allowed[None], raw_scores, masked_score)

    lse_list = []
    mixed_parts = []
    attn_branch_parts = []
    for c in range(CHUNKS):
        block_scores = scores_block(c)
        row_top = jnp.max(block_scores, -1, keepdims=True)
        exp_scores = jnp.exp(block_scores - row_top)
        row_total = jnp.sum(exp_scores, -1, keepdims=True)
        prob_rows = exp_scores / row_total
        lse_list.append(row_top + jnp.log(row_total))
        heads_out = jnp.einsum(
            "hts,shd->thd",
            prob_rows.astype(jnp.bfloat16),
            value,
            preferred_element_type=jnp.float32,
        )
        mixed = (
            (heads_out * head_on_parts[c][:, None, None])
            .astype(jnp.bfloat16)
            .reshape(chunk_rows, local_dim)
        )
        mixed_parts.append(mixed)
        attn_branch_parts.append(
            scatter_rows(
                jnp.dot(mixed, w_out, preferred_element_type=jnp.float32).astype(jnp.bfloat16)
            )
        )
    x_parts = cut(x_rows)
    scale_head_own = cut(own_scale_head)
    scale_ffn_own = cut(own_scale_ffn)
    grad_out = cotangent.astype(jnp.float32)
    grad_out_parts = cut(grad_out)
    own_hot_parts = cut(own_hot)
    mid_parts = []
    norm2_parts = []
    h_two_parts = []
    for c in range(CHUNKS):
        mid_rows = x_parts[c] + scale_head_own[c] * attn_branch_parts[c]
        normed2, unit2, inv_std2 = norm_rows(mid_rows, ln2_gain, ln2_bias)
        mid_parts.append(mid_rows)
        norm2_parts.append((unit2, inv_std2))
        h_two_parts.append(gather_rows(normed2.astype(jnp.bfloat16)))
    hidden_parts = []
    ffn_grad_parts = []
    grad_up_parts = []
    normed2_grad_parts = []
    normed2_sent = []
    for c in range(CHUNKS):
        ffn_grad = (scale_ffn_parts[c] * cotangent_parts[c].astype(jnp.float32)).astype(
            jnp.bfloat16
        )
        hidden_grad = jnp.dot(ffn_grad, w_down.T, preferred_element_type=jnp.float32).astype(
            jnp.bfloat16
        )
        up_proj = jnp.dot(h_two_parts[c], w_up, preferred_element_type=jnp.float32)
        relu_rows = jnp.maximum(up_proj, 0.0)
        on_rows = ffn_on_parts[c][:, None]
        hidden_parts.append((relu_rows * relu_rows * on_rows).astype(jnp.bfloat16))
        grad_up = (hidden_grad.astype(jnp.float32) * (2.0 * relu_rows * on_rows)).astype(
            jnp.bfloat16
        )
        ffn_grad_parts.append(ffn_grad)
        grad_up_parts.append(grad_up)
        normed2_sent.append(
            jnp.dot(grad_up, w_up.T, preferred_element_type=jnp.float32).astype(jnp.bfloat16)
        )
        normed2_grad_parts.append(send_rows(normed2_sent[c]))
    hidden_parts, ffn_grad_parts, grad_up_parts, h_two_parts, _ = lax.optimization_barrier(
        (hidden_parts, ffn_grad_parts, grad_up_parts, h_two_parts, normed2_sent)
    )
    hidden_all = jnp.concatenate(hidden_parts, 0)
    ffn_grad_all = jnp.concatenate(ffn_grad_parts, 0)
    grad_up_all = jnp.concatenate(grad_up_parts, 0)
    h_two_all = jnp.concatenate(h_two_parts, 0)
    down_full = jnp.dot(
        hidden_all.T, ffn_grad_all, preferred_element_type=jnp.float32
    ).astype(jnp.bfloat16)
    up_full = jnp.dot(h_two_all.T, grad_up_all, preferred_element_type=jnp.float32).astype(
        jnp.bfloat16
    )
    normed2_grad_parts, _, _ = lax.optimization_barrier((normed2_grad_parts, down_full, up_full))
    normed2_grad_parts = [sum_parts(parts) for parts in normed2_grad_parts]
    mid_grad_parts = []
    attn_grad_sent = []
    gain2_grad = 0.0
    bias2_grad = 0.0
    part_head = 0.0
    for c in range(CHUNKS):
        unit2, inv_std2 = norm2_parts[c]
        back_two, gain_part, bias_part = norm_back(
            normed2_grad_parts[c], unit2, inv_std2, ln2_gain
        )
        gain2_grad = gain2_grad + gain_part
        bias2_grad = bias2_grad + bias_part
        mid_grad = grad_out_parts[c] + back_two
        part_head = part_head + jnp.sum(
            own_hot_parts[c] * jnp.sum(mid_grad * attn_branch_parts[c], 1, keepdims=True), 0
        )
        mid_grad_parts.append(mid_grad)
        attn_grad_sent.append((scale_head_own[c] * mid_grad).astype(jnp.bfloat16))
    attn_grad_parts = [gather_rows(part) for part in attn_grad_sent]
    hidden_late, _ = lax.optimization_barrier((hidden_all, attn_grad_sent))
    ffn_full = jnp.dot(hidden_late, w_down, preferred_element_type=jnp.float32).astype(jnp.bfloat16)
    down_part = scatter_groups(down_full, 1)
    up_part = scatter_groups(up_full, 0)
    attn_grad_parts, ffn_full, down_part, up_part = lax.optimization_barrier(
        (attn_grad_parts, ffn_full, down_part, up_part)
    )
    blocks = ffn_full.reshape(CHUNKS, shard_count, part_rows, D)[:, ::-1]
    blocks = lax.dynamic_slice_in_dim(
        jnp.concatenate([blocks, blocks], 1), shard_count - 1 - mp_index, shard_count, 1
    )
    ffn_branch = lax.psum_scatter(
        blocks.transpose(1, 0, 2, 3).reshape(group_rows, D), "mp", scatter_dimension=0, tiled=True
    )
    early_sums = sum_all(jnp.stack([gain2_grad, bias2_grad]))
    key_grad = 0.0
    value_grad = 0.0
    query_grads = []
    for c in range(CHUNKS):
        grad_blk = (
            jnp.dot(attn_grad_parts[c], w_out.T, preferred_element_type=jnp.float32)
            .astype(jnp.bfloat16)
            .reshape(chunk_rows, heads_here, HEAD_DIM)
        ) * head_on_parts[c].astype(jnp.bfloat16)[:, None, None]
        block_scores = scores_block(c)
        prob_rows = jnp.exp(block_scores - lse_list[c])
        prob_grad = jnp.einsum("thd,shd->hts", grad_blk, value, preferred_element_type=jnp.float32)
        delta = jnp.sum(prob_rows * prob_grad, -1, keepdims=True)
        score_grad = (prob_rows * (prob_grad - delta)).astype(jnp.bfloat16)
        query_grads.append(
            jnp.einsum("hts,shd->thd", score_grad, key_rows, preferred_element_type=jnp.float32)
            * inv_root
        )
        key_grad = (
            key_grad
            + jnp.einsum(
                "hts,thd->shd", score_grad, query_parts[c], preferred_element_type=jnp.float32
            )
            * inv_root
        )
        value_grad = value_grad + jnp.einsum(
            "hts,thd->shd",
            prob_rows.astype(jnp.bfloat16),
            grad_blk,
            preferred_element_type=jnp.float32,
        )
    query_grad = jnp.concatenate(query_grads, 0)
    qkv_grad = jnp.stack(
        [
            rotate_back(query_grad, cosine_b, sine_b),
            rotate_back(key_grad, cosine_b, sine_b),
            value_grad,
        ],
        1,
    )
    qkv_grad = qkv_grad.astype(jnp.bfloat16).reshape(group_rows, 3 * local_dim)
    qkv_grad, mixed_late = lax.optimization_barrier((qkv_grad, mixed_parts))
    out_full = jnp.dot(
        jnp.concatenate(mixed_late, 0).T,
        jnp.concatenate(attn_grad_parts, 0),
        preferred_element_type=jnp.float32,
    ).astype(jnp.bfloat16)
    normed1_sent = [
        jnp.dot(part, w_qkv_flat.T, preferred_element_type=jnp.float32).astype(jnp.bfloat16)
        for part in cut_all(qkv_grad)
    ]
    normed1_sent, early_sums, ffn_branch, _ = lax.optimization_barrier(
        (normed1_sent, early_sums, ffn_branch, out_full)
    )
    out_part = scatter_groups(out_full, 1)
    ffn_branch = ffn_branch.astype(jnp.float32)
    mid_all = jnp.concatenate(mid_parts, 0)
    block_out = (mid_all + own_scale_ffn * ffn_branch).astype(jnp.bfloat16)
    part_ffn = jnp.sum(own_hot * jnp.sum(grad_out * ffn_branch, 1, keepdims=True), 0)
    scale_grads = sum_over(jnp.stack([part_head, part_ffn]), "mp")
    logit_head_grad = (scale_grads[0] * scale_head)[:, None] * (pick_head - prob_head)
    logit_ffn_grad = (scale_grads[1] * scale_ffn)[:, None] * (pick_ffn - prob_ffn)
    logit_grad = jnp.concatenate([logit_head_grad, logit_ffn_grad], 1)
    router_part = jnp.dot(logit_grad.T, slot_means, precision=lax.Precision.HIGHEST) / shard_count
    mean_grad = jnp.dot(logit_grad, w_router.T, precision=lax.Precision.HIGHEST) / counts[:, None]
    normed1_parts = [send_rows(part) for part in normed1_sent]
    qkv_late, _ = lax.optimization_barrier((qkv_grad, normed1_sent))
    qkv_full = (
        jnp.dot(h_one_all.T, qkv_late, preferred_element_type=jnp.float32)
        .astype(jnp.bfloat16)
        .reshape(D, 3, local_dim)
    )
    normed1_parts, _ = lax.optimization_barrier((normed1_parts, qkv_full))
    normed1_grad = jnp.concatenate([sum_parts(parts) for parts in normed1_parts], 0)
    qkv_weight_grad = scatter_groups(qkv_full, 0)
    normed1_grad = normed1_grad + jnp.dot(own_hot, mean_grad, precision=lax.Precision.HIGHEST)
    back_one, gain1_grad, bias1_grad = norm_back(normed1_grad, unit1, inv_std1, ln1_gain)
    input_grad = (jnp.concatenate(mid_grad_parts, 0) + back_one).astype(jnp.bfloat16)
    late_sums = sum_all(
        jnp.concatenate([gain1_grad[None], bias1_grad[None], router_part], 0)
    )
    return (
        block_out,
        input_grad,
        late_sums[0],
        late_sums[1],
        qkv_weight_grad.astype(jnp.float32),
        out_part.astype(jnp.float32),
        early_sums[0],
        early_sums[1],
        up_part.astype(jnp.float32),
        down_part.astype(jnp.float32),
        late_sums[2:].T,
    )


def solution(mesh):
    placed = (
        P(("dp", "mp"), None),
        P(("dp", "mp"), None),
        P(),
        P(),
        P(None, None, "mp"),
        P("mp", None),
        P(),
        P(),
        P(None, "mp"),
        P("mp", None),
        P(),
        P("dp"),
        P("dp"),
        P("dp"),
    )
    return jax.shard_map(
        local,
        mesh=mesh,
        in_specs=placed,
        out_specs=(
            P(("dp", "mp"), None),
            P(("dp", "mp"), None),
            P(),
            P(),
            P("dp", None, "mp"),
            P("mp", "dp"),
            P(),
            P(),
            P("dp", "mp"),
            P("mp", "dp"),
            P(),
        ),
        check_vma=False,
    )
```

```python
import functools
import math

import jax
import jax.numpy as jnp
from jax import lax
from jax.experimental import pallas as pl
from jax.experimental.pallas import tpu as pltpu
from jax.sharding import PartitionSpec as P

D = 2048
HEAD_DIM = 128
PIECES = 4
MESH = pl.DeviceIdType.MESH


epsilon = 1e-05
masked_score = -1000000000.0


def norm_rows(values, gain_vec, bias_vec):
    center = values - jnp.mean(values, -1, keepdims=True)
    inv_std = lax.rsqrt(jnp.mean(center * center, -1, keepdims=True) + epsilon)
    unit_rows = center * inv_std
    return (unit_rows * gain_vec + bias_vec, unit_rows, inv_std)


def norm_back(grad_rows, unit_rows, inv_std, gain_vec):
    scaled = grad_rows * gain_vec
    inner = (
        scaled
        - jnp.mean(scaled, -1, keepdims=True)
        - unit_rows * jnp.mean(scaled * unit_rows, -1, keepdims=True)
    )
    return (inner * inv_std, jnp.sum(grad_rows * unit_rows, 0), jnp.sum(grad_rows, 0))


def rotary_tables(positions, full_width):
    half_width = full_width // 2
    frequency = jnp.exp(
        jnp.arange(half_width, dtype=jnp.float32) * (-2.0 * math.log(10000.0) / full_width)
    )
    angles = positions[:, None] * frequency[None, :]
    cosine = jnp.cos(angles)
    sine_rows = jnp.sin(angles)
    return (jnp.concatenate([cosine, cosine], -1), jnp.concatenate([sine_rows, sine_rows], -1))


def rotate(values, cosine, sine_rows):
    half_width = values.shape[-1] // 2
    turned = jnp.concatenate([-values[..., half_width:], values[..., :half_width]], -1)
    return values * cosine + turned * sine_rows


def rotate_back(grad_rows, cosine, sine_rows):
    half_width = grad_rows.shape[-1] // 2
    moved = grad_rows * sine_rows
    turned = jnp.concatenate([moved[..., half_width:], -moved[..., :half_width]], -1)
    return grad_rows * cosine + turned


def row_loop(first, count, step, run):
    def one(index, carry):
        run(pl.ds(pl.multiple_of(first + index * step, step), step))
        return carry

    lax.fori_loop(0, count // step, one, 0)


def exchange_kernel(size, finish, count, *refs):
    part, inputs = refs[0], refs[1 : 1 + count]
    gathered, outputs = refs[1 + count], refs[2 + count : -8]
    from_left, from_right = refs[-8:-6]
    right_sent, right_got, left_sent, left_got, all_sent, all_got = refs[-6:]
    me = lax.axis_index("mp")
    rows_here = part.shape[1]
    piece = rows_here // PIECES
    last = size - 1

    barrier = pltpu.get_barrier_semaphore()
    for shift in range(1, size):
        pl.semaphore_signal(
            barrier, 1, device_id={"mp": lax.rem(me + shift, size)}, device_id_type=MESH
        )
    pl.semaphore_wait(barrier, size - 1)

    def rows_of(c):
        return pl.ds(pl.multiple_of(c * piece, piece), piece)

    def to_right(source, target, c):
        return pltpu.make_async_remote_copy(
            src_ref=source.at[target, rows_of(c)],
            dst_ref=from_left.at[target, rows_of(c)],
            send_sem=right_sent.at[target, c],
            recv_sem=right_got.at[target, c],
            device_id={"mp": lax.rem(me + 1, size)},
            device_id_type=MESH,
        )

    def to_left(source, target, c):
        return pltpu.make_async_remote_copy(
            src_ref=source.at[target, rows_of(c)],
            dst_ref=from_right.at[target, rows_of(c)],
            send_sem=left_sent.at[target, c],
            recv_sem=left_got.at[target, c],
            device_id={"mp": lax.rem(me + last, size)},
            device_id_type=MESH,
        )

    def to_all(shift, owner, c):
        peer = lax.rem(me + shift, size)
        return pltpu.make_async_remote_copy(
            src_ref=gathered.at[owner, rows_of(c)],
            dst_ref=gathered.at[owner, rows_of(c)],
            send_sem=all_sent.at[shift, c],
            recv_sem=all_got.at[owner, c],
            device_id={"mp": peer},
            device_id_type=MESH,
        )

    def add_into(held, target, c):
        def run(rows):
            held[target, rows, :] = (
                held[target, rows, :].astype(jnp.float32)
                + part[target, rows, :].astype(jnp.float32)
            ).astype(jnp.bfloat16)

        row_loop(c * piece, piece, 16, run)

    def relay(c):
        for far in range(size - 1):
            target = last - far

            @pl.when(me == 0)
            def _():
                to_right(part, target, c).start()

            @pl.when((me > 0) & (me < target))
            def _():
                to_right(from_left, target, c).wait_recv()
                add_into(from_left, target, c)
                to_right(from_left, target, c).start()

            @pl.when(me == last)
            def _():
                to_left(part, far, c).start()

            @pl.when((me < last) & (me > far))
            def _():
                to_left(from_right, far, c).wait_recv()
                add_into(from_right, far, c)
                to_left(from_right, far, c).start()

    def close(c):
        @pl.when(me > 0)
        def _():
            to_right(from_left, me, c).wait_recv()

        @pl.when(me < last)
        def _():
            to_left(from_right, me, c).wait_recv()

        def run(rows):
            total = part[me, rows, :].astype(jnp.float32)
            total = total + from_left[me, rows, :].astype(jnp.float32)
            total = total + from_right[me, rows, :].astype(jnp.float32)
            gathered[me, rows, :] = finish(total, rows, inputs, outputs)

        row_loop(c * piece, piece, 16, run)
        for shift in range(1, size):
            to_all(shift, me, c).start()

    def clear(held, slot):
        def run(rows):
            held[slot, rows, :] = jnp.zeros((16, held.shape[2]), jnp.bfloat16)

        row_loop(0, rows_here, 16, run)

    @pl.when(me == 0)
    def _():
        clear(from_left, 0)

    @pl.when(me == last)
    def _():
        clear(from_right, last)

    for out in outputs[1:]:
        out[...] = jnp.zeros_like(out)
    relay(0)

    def step(c, carry):
        relay(c + 1)
        close(c)
        return carry

    lax.fori_loop(0, PIECES - 1, step, 0)
    close(PIECES - 1)

    def drain(c, carry):
        for shift in range(1, size):
            to_all(shift, lax.rem(me + shift, size), c).wait_recv()
            to_all(shift, me, c).wait_send()
        for target in range(1, size):

            @pl.when(me < target)
            def _():
                to_right(from_left, target, c).wait_send()

        for target in range(size - 1):

            @pl.when(me > target)
            def _():
                to_left(from_right, target, c).wait_send()

        return carry

    lax.fori_loop(0, PIECES, drain, 0)


def exchange(finish, partial, inputs, outputs, number):
    size = lax.axis_size("mp")
    part = partial.reshape(size, partial.shape[0] // size, D)
    vmem = pl.BlockSpec(memory_space=pltpu.VMEM)
    got = pl.pallas_call(
        functools.partial(exchange_kernel, size, finish, len(inputs)),
        out_shape=[jax.ShapeDtypeStruct(part.shape, jnp.bfloat16), *outputs],
        in_specs=[vmem] * (1 + len(inputs)),
        out_specs=[vmem] * (1 + len(outputs)),
        scratch_shapes=[pltpu.VMEM(part.shape, jnp.bfloat16)] * 2
        + [pltpu.SemaphoreType.DMA((size, PIECES))] * 6,
        compiler_params=pltpu.CompilerParams(
            collective_id=number, has_side_effects=True, vmem_limit_bytes=48 << 20
        ),
        cost_estimate=pl.CostEstimate(
            flops=30 * part.size, bytes_accessed=100 * part.size, transcendentals=0
        ),
    )(part, *inputs)
    return got[0].reshape(partial.shape), *got[1:]


def lane_mean(values):
    return jnp.sum(values, -1, keepdims=True) * (1.0 / values.shape[-1])


def finish_forward(total, rows, inputs, outputs):
    tokens, scale, gain, bias = inputs
    outputs[0][rows, :] = total
    mid = tokens[rows, :].astype(jnp.float32) + scale[rows, :] * total
    center = mid - lane_mean(mid)
    unit = center * lax.rsqrt(lane_mean(center * center) + epsilon)
    return (unit * gain[...] + bias[...]).astype(jnp.bfloat16)


def finish_backward(total, rows, inputs, outputs):
    tokens, scale, gain, branch, cotangent = inputs
    mid = tokens[rows, :].astype(jnp.float32) + scale[rows, :] * branch[rows, :]
    center = mid - lane_mean(mid)
    inv_std = lax.rsqrt(lane_mean(center * center) + epsilon)
    unit = center * inv_std
    outputs[1][0:1, :] += jnp.sum(total * unit, 0, keepdims=True)
    outputs[1][1:2, :] += jnp.sum(total, 0, keepdims=True)
    scaled = total * gain[...]
    inner = scaled - lane_mean(scaled) - unit * lane_mean(scaled * unit)
    mid_grad = cotangent[rows, :].astype(jnp.float32) + inv_std * inner
    outputs[0][rows, :] = mid_grad
    return (scale[rows, :] * mid_grad).astype(jnp.bfloat16)


def scatter_rows(partial):
    shard_count = lax.axis_size("mp")
    me = lax.axis_index("mp")
    rows = partial.shape[0] // shard_count
    parts = [lax.dynamic_slice_in_dim(partial, me * rows, rows)]
    for shift in range(1, shard_count):
        pairs = [(holder, (holder - shift) % shard_count) for holder in range(shard_count)]
        owner = lax.rem(me - shift + shard_count, shard_count)
        sent = lax.dynamic_slice_in_dim(partial, owner * rows, rows)
        parts.append(lax.ppermute(sent, "mp", pairs))
    return parts


def sum_parts(parts):
    total = parts[0].astype(jnp.float32)
    for part in parts[1:]:
        total = total + part.astype(jnp.float32)
    return total


def scatter_groups(values, dim):
    return lax.psum_scatter(values, "dp", scatter_dimension=dim, tiled=True)


def sum_over(values, axis_name):
    size = lax.axis_size(axis_name)
    for bit in range(size.bit_length() - 1):
        pairs = [(one, one ^ (1 << bit)) for one in range(size)]
        values = values + lax.ppermute(values, axis_name, pairs)
    return values


def local(
    tokens,
    cotangent,
    ln1_gain,
    ln1_bias,
    w_qkv,
    w_out,
    ln2_gain,
    ln2_bias,
    w_up,
    w_down,
    w_router,
    seq_first,
    head_width,
    ffn_width,
):
    shard_count = lax.axis_size("mp")
    mp_index = lax.axis_index("mp")
    tok_dev = tokens.shape[0]
    group_rows = tok_dev * shard_count
    local_dim = w_qkv.shape[2]
    heads_here = local_dim // HEAD_DIM
    split_at = seq_first[0]
    row_ids = jnp.arange(group_rows, dtype=jnp.int32)
    row_slot = (row_ids >= split_at).astype(jnp.int32)
    positions = (row_ids - row_slot * split_at).astype(jnp.float32)
    slot_hot = (row_slot[None, :] == jnp.arange(2, dtype=jnp.int32)[:, None]).astype(jnp.float32)
    counts = jnp.maximum(jnp.sum(slot_hot, 1), 1.0)
    own_rows = mp_index * tok_dev + jnp.arange(tok_dev, dtype=jnp.int32)
    own_slot = (own_rows >= split_at).astype(jnp.int32)
    own_hot = (own_slot[:, None] == jnp.arange(2, dtype=jnp.int32)[None, :]).astype(jnp.float32)
    head_on = (mp_index < jnp.where(row_slot == 1, head_width[1], head_width[0])).astype(
        jnp.float32
    )
    ffn_on = (mp_index < jnp.where(row_slot == 1, ffn_width[1], ffn_width[0])).astype(jnp.float32)
    x_rows = tokens.astype(jnp.float32)
    normed1, unit1, inv_std1 = norm_rows(x_rows, ln1_gain, ln1_bias)
    h_one = normed1.astype(jnp.bfloat16)
    h_one_all = lax.all_gather(h_one, "mp", axis=0, tiled=True)
    h_one_all, late_cotangent = lax.optimization_barrier((h_one_all, cotangent))
    cotangent_all = lax.all_gather(late_cotangent, "mp", axis=0, tiled=True)
    slot_means = (
        jnp.dot(slot_hot.astype(jnp.bfloat16), h_one_all, preferred_element_type=jnp.float32)
        / counts[:, None]
    )
    logits = jnp.dot(slot_means, w_router, precision=lax.Precision.HIGHEST)
    levels = jnp.arange(shard_count, dtype=jnp.int32)
    pick_head = (levels[None, :] == head_width[:, None] - 1).astype(jnp.float32)
    pick_ffn = (levels[None, :] == ffn_width[:, None] - 1).astype(jnp.float32)
    prob_head = jax.nn.softmax(logits[:, :shard_count], -1)
    prob_ffn = jax.nn.softmax(logits[:, shard_count:], -1)
    scale_head = shard_count * jnp.sum(prob_head * pick_head, 1)
    scale_ffn = shard_count * jnp.sum(prob_ffn * pick_ffn, 1)
    own_scale_head = jnp.where(own_slot == 1, scale_head[1], scale_head[0])[:, None]
    own_scale_ffn = jnp.where(own_slot == 1, scale_ffn[1], scale_ffn[0])[:, None]
    w_qkv_flat = w_qkv.reshape(D, 3 * local_dim)
    qkv_rows = jnp.dot(h_one_all, w_qkv_flat, preferred_element_type=jnp.float32).reshape(
        group_rows, 3, heads_here, HEAD_DIM
    )
    cosine, sine_rows = rotary_tables(positions, HEAD_DIM)
    cosine_b = cosine[:, None, :]
    sine_b = sine_rows[:, None, :]
    query = rotate(qkv_rows[:, 0], cosine_b, sine_b).astype(jnp.bfloat16)
    key_rows = rotate(qkv_rows[:, 1], cosine_b, sine_b).astype(jnp.bfloat16)
    value = qkv_rows[:, 2].astype(jnp.bfloat16)
    inv_root = 1.0 / math.sqrt(HEAD_DIM)
    row_block = min(512, group_rows)

    def scores_block(offset):
        stop = offset + row_block
        query_blk = query[offset : offset + row_block]
        raw_scores = (
            jnp.einsum("thd,shd->hts", query_blk, key_rows[:stop], preferred_element_type=jnp.float32)
            * inv_root
        )
        allowed = (row_slot[offset:stop, None] == row_slot[None, :stop]) & (
            row_ids[None, :stop] <= row_ids[offset:stop, None]
        )
        return jnp.where(allowed[None], raw_scores, masked_score)

    out_list = []
    lse_list = []
    for offset in range(0, group_rows, row_block):
        block_scores = scores_block(offset)
        row_top = jnp.max(block_scores, -1, keepdims=True)
        exp_scores = jnp.exp(block_scores - row_top)
        row_total = jnp.sum(exp_scores, -1, keepdims=True)
        prob_rows = exp_scores / row_total
        lse_list.append(row_top + jnp.log(row_total))
        out_list.append(
            jnp.einsum(
                "hts,shd->thd",
                prob_rows.astype(jnp.bfloat16),
                value[: offset + row_block],
                preferred_element_type=jnp.float32,
            )
        )
    heads_out = jnp.concatenate(out_list, 0)
    attn_mixed = (
        (heads_out * head_on[:, None, None]).astype(jnp.bfloat16).reshape(group_rows, local_dim)
    )
    attn_sent = jnp.dot(attn_mixed, w_out, preferred_element_type=jnp.float32).astype(jnp.bfloat16)
    h_two_all, attn_branch = exchange(
        finish_forward,
        attn_sent,
        (tokens, own_scale_head, ln2_gain[None], ln2_bias[None]),
        (jax.ShapeDtypeStruct((tok_dev, D), jnp.float32),),
        0,
    )
    up_proj = jnp.dot(h_two_all, w_up, preferred_element_type=jnp.float32)
    relu_rows = jnp.maximum(up_proj, 0.0)
    hidden = (relu_rows * relu_rows * ffn_on[:, None]).astype(jnp.bfloat16)
    row_scale_ffn = jnp.where(row_slot == 1, scale_ffn[1], scale_ffn[0])[:, None]
    ffn_grad_all = (row_scale_ffn * cotangent_all.astype(jnp.float32)).astype(jnp.bfloat16)
    hidden_grad = jnp.dot(ffn_grad_all, w_down.T, preferred_element_type=jnp.float32).astype(
        jnp.bfloat16
    )
    grad_up = (hidden_grad.astype(jnp.float32) * (2.0 * relu_rows * ffn_on[:, None])).astype(
        jnp.bfloat16
    )
    normed2_sent = jnp.dot(grad_up, w_up.T, preferred_element_type=jnp.float32).astype(
        jnp.bfloat16
    )
    down_full = jnp.dot(hidden.T, ffn_grad_all, preferred_element_type=jnp.float32).astype(
        jnp.bfloat16
    )
    up_full = jnp.dot(h_two_all.T, grad_up, preferred_element_type=jnp.float32).astype(
        jnp.bfloat16
    )
    down_part = scatter_groups(down_full, 1)
    up_part = scatter_groups(up_full, 0)
    normed2_sent, _, _ = lax.optimization_barrier((normed2_sent, down_full, up_full))
    attn_grad_all, mid_grad, sums2 = exchange(
        finish_backward,
        normed2_sent,
        (tokens, own_scale_head, ln2_gain[None], attn_branch, cotangent),
        (
            jax.ShapeDtypeStruct((tok_dev, D), jnp.float32),
            jax.ShapeDtypeStruct((8, D), jnp.float32),
        ),
        1,
    )
    hidden_late, _ = lax.optimization_barrier((hidden, attn_grad_all))
    ffn_sent = jnp.dot(hidden_late, w_down, preferred_element_type=jnp.float32).astype(
        jnp.bfloat16
    )
    mixed_grad = (
        jnp.dot(attn_grad_all, w_out.T, preferred_element_type=jnp.float32)
        .astype(jnp.bfloat16)
        .reshape(group_rows, heads_here, HEAD_DIM)
    )
    mixed_grad = mixed_grad * head_on.astype(jnp.bfloat16)[:, None, None]
    key_grad = 0.0
    value_grad = 0.0

    def at_front(values):
        return jnp.pad(values, ((0, group_rows - values.shape[0]), (0, 0), (0, 0)))

    query_grads = []
    for block_num, offset in enumerate(range(0, group_rows, row_block)):
        block_scores = scores_block(offset)
        prob_rows = jnp.exp(block_scores - lse_list[block_num])
        stop = offset + row_block
        if stop == group_rows:
            mixed_grad, ffn_sent, down_part, up_part = lax.optimization_barrier(
                (mixed_grad, ffn_sent, down_part, up_part)
            )
        grad_blk = mixed_grad[offset:stop]
        prob_grad = jnp.einsum("thd,shd->hts", grad_blk, value[:stop], preferred_element_type=jnp.float32)
        delta = jnp.sum(prob_rows * prob_grad, -1, keepdims=True)
        score_grad = (prob_rows * (prob_grad - delta)).astype(jnp.bfloat16)
        query_grads.append(
            jnp.einsum("hts,shd->thd", score_grad, key_rows[:stop], preferred_element_type=jnp.float32)
            * inv_root
        )
        key_grad = (
            key_grad
            + at_front(
                jnp.einsum(
                    "hts,thd->shd",
                    score_grad,
                    query[offset:stop],
                    preferred_element_type=jnp.float32,
                )
            )
            * inv_root
        )
        value_grad = value_grad + at_front(
            jnp.einsum(
                "hts,thd->shd",
                prob_rows.astype(jnp.bfloat16),
                grad_blk,
                preferred_element_type=jnp.float32,
            )
        )
    query_grad = jnp.concatenate(query_grads, 0)
    qkv_grad = jnp.stack(
        [
            rotate_back(query_grad, cosine_b, sine_b),
            rotate_back(key_grad, cosine_b, sine_b),
            value_grad,
        ],
        1,
    )
    qkv_grad = qkv_grad.astype(jnp.bfloat16).reshape(group_rows, 3 * local_dim)
    normed1_sent = jnp.dot(qkv_grad, w_qkv_flat.T, preferred_element_type=jnp.float32).astype(
        jnp.bfloat16
    )
    normed1_parts = scatter_rows(normed1_sent)
    qkv_late, mixed_late, _ = lax.optimization_barrier((qkv_grad, attn_mixed, normed1_sent))
    qkv_full = (
        jnp.dot(h_one_all.T, qkv_late, preferred_element_type=jnp.float32)
        .astype(jnp.bfloat16)
        .reshape(D, 3, local_dim)
    )
    out_full = jnp.dot(mixed_late.T, attn_grad_all, preferred_element_type=jnp.float32).astype(
        jnp.bfloat16
    )
    ffn_branch = lax.psum_scatter(ffn_sent, "mp", scatter_dimension=0, tiled=True)
    qkv_full, out_full, ffn_branch = lax.optimization_barrier((qkv_full, out_full, ffn_branch))
    ffn_branch = ffn_branch.astype(jnp.float32)
    qkv_part = scatter_groups(qkv_full, 0)
    out_part = scatter_groups(out_full, 1)
    mid_rows = x_rows + own_scale_head * attn_branch
    block_out = (mid_rows + own_scale_ffn * ffn_branch).astype(jnp.bfloat16)
    part_head = jnp.sum(own_hot * jnp.sum(mid_grad * attn_branch, 1, keepdims=True), 0)
    part_ffn = jnp.sum(
        own_hot * jnp.sum(cotangent.astype(jnp.float32) * ffn_branch, 1, keepdims=True), 0
    )
    scale_grads = sum_over(jnp.stack([part_head, part_ffn]), "mp")
    normed1_grad = sum_parts(normed1_parts)
    logit_head_grad = (scale_grads[0] * scale_head)[:, None] * (pick_head - prob_head)
    logit_ffn_grad = (scale_grads[1] * scale_ffn)[:, None] * (pick_ffn - prob_ffn)
    logit_grad = jnp.concatenate([logit_head_grad, logit_ffn_grad], 1)
    router_part = jnp.dot(logit_grad.T, slot_means, precision=lax.Precision.HIGHEST) / shard_count
    mean_grad = jnp.dot(logit_grad, w_router.T, precision=lax.Precision.HIGHEST) / counts[:, None]
    normed1_grad = normed1_grad + jnp.dot(own_hot, mean_grad, precision=lax.Precision.HIGHEST)
    back_one, gain1_grad, bias1_grad = norm_back(normed1_grad, unit1, inv_std1, ln1_gain)
    input_grad = (mid_grad + back_one).astype(jnp.bfloat16)
    packed = jnp.concatenate([gain1_grad[None], bias1_grad[None], sums2[:2], router_part], 0)
    packed = sum_over(sum_over(packed, "mp"), "dp")
    return (
        block_out,
        input_grad,
        packed[0],
        packed[1],
        qkv_part.astype(jnp.float32),
        out_part.astype(jnp.float32),
        packed[2],
        packed[3],
        up_part.astype(jnp.float32),
        down_part.astype(jnp.float32),
        packed[4:].T,
    )


def solution(mesh):
    placed = (
        P(("dp", "mp"), None),
        P(("dp", "mp"), None),
        P(),
        P(),
        P(None, None, "mp"),
        P("mp", None),
        P(),
        P(),
        P(None, "mp"),
        P("mp", None),
        P(),
        P("dp"),
        P("dp"),
        P("dp"),
    )
    return jax.shard_map(
        local,
        mesh=mesh,
        in_specs=placed,
        out_specs=(
            P(("dp", "mp"), None),
            P(("dp", "mp"), None),
            P(),
            P(),
            P("dp", None, "mp"),
            P("mp", "dp"),
            P(),
            P(),
            P("dp", "mp"),
            P("mp", "dp"),
            P(),
        ),
        check_vma=False,
    )
```

```python
import functools
import math

import jax
import jax.numpy as jnp
from jax import lax
from jax.experimental import pallas as pl
from jax.experimental.pallas import tpu as pltpu
from jax.sharding import PartitionSpec as P

D = 2048
HEAD_DIM = 128
PIECES = 8
MESH = pl.DeviceIdType.MESH


epsilon = 1e-05
masked_score = -1000000000.0


def norm_rows(values, gain_vec, bias_vec):
    center = values - jnp.mean(values, -1, keepdims=True)
    inv_std = lax.rsqrt(jnp.mean(center * center, -1, keepdims=True) + epsilon)
    unit_rows = center * inv_std
    return (unit_rows * gain_vec + bias_vec, unit_rows, inv_std)


def norm_back(grad_rows, unit_rows, inv_std, gain_vec):
    scaled = grad_rows * gain_vec
    inner = (
        scaled
        - jnp.mean(scaled, -1, keepdims=True)
        - unit_rows * jnp.mean(scaled * unit_rows, -1, keepdims=True)
    )
    return (inner * inv_std, jnp.sum(grad_rows * unit_rows, 0), jnp.sum(grad_rows, 0))


def rotary_tables(positions, full_width):
    half_width = full_width // 2
    frequency = jnp.exp(
        jnp.arange(half_width, dtype=jnp.float32) * (-2.0 * math.log(10000.0) / full_width)
    )
    angles = positions[:, None] * frequency[None, :]
    cosine = jnp.cos(angles)
    sine_rows = jnp.sin(angles)
    return (jnp.concatenate([cosine, cosine], -1), jnp.concatenate([sine_rows, sine_rows], -1))


def rotate(values, cosine, sine_rows):
    half_width = values.shape[-1] // 2
    turned = jnp.concatenate([-values[..., half_width:], values[..., :half_width]], -1)
    return values * cosine + turned * sine_rows


def rotate_back(grad_rows, cosine, sine_rows):
    half_width = grad_rows.shape[-1] // 2
    moved = grad_rows * sine_rows
    turned = jnp.concatenate([moved[..., half_width:], -moved[..., :half_width]], -1)
    return grad_rows * cosine + turned


def row_loop(first, count, step, run):
    def one(index, carry):
        run(pl.ds(pl.multiple_of(first + index * step, step), step))
        return carry

    lax.fori_loop(0, count // step, one, 0)


def exchange_kernel(size, finish, count, spread, *refs):
    part, inputs = refs[0], refs[1 : 1 + count]
    gathered, outputs = refs[1 + count], refs[2 + count : -9]
    from_left, from_right = refs[-9:-7]
    right_sent, right_got, left_sent, left_got, ahead_sent, back_sent, all_got = refs[-7:]
    me = lax.axis_index("mp")
    rows_here = part.shape[1]
    piece = rows_here // PIECES
    last = size - 1

    barrier = pltpu.get_barrier_semaphore()
    for shift in range(1, size):
        pl.semaphore_signal(
            barrier, 1, device_id={"mp": lax.rem(me + shift, size)}, device_id_type=MESH
        )
    pl.semaphore_wait(barrier, size - 1)

    def rows_of(c):
        return pl.ds(pl.multiple_of(c * piece, piece), piece)

    def to_right(source, target, c):
        return pltpu.make_async_remote_copy(
            src_ref=source.at[target, rows_of(c)],
            dst_ref=from_left.at[target, rows_of(c)],
            send_sem=right_sent.at[target, c],
            recv_sem=right_got.at[target, c],
            device_id={"mp": lax.rem(me + 1, size)},
            device_id_type=MESH,
        )

    def to_left(source, target, c):
        return pltpu.make_async_remote_copy(
            src_ref=source.at[target, rows_of(c)],
            dst_ref=from_right.at[target, rows_of(c)],
            send_sem=left_sent.at[target, c],
            recv_sem=left_got.at[target, c],
            device_id={"mp": lax.rem(me + last, size)},
            device_id_type=MESH,
        )

    def spread_right(owner, c):
        return pltpu.make_async_remote_copy(
            src_ref=gathered.at[owner, rows_of(c)],
            dst_ref=gathered.at[owner, rows_of(c)],
            send_sem=ahead_sent.at[owner, c],
            recv_sem=all_got.at[owner, c],
            device_id={"mp": lax.rem(me + 1, size)},
            device_id_type=MESH,
        )

    def spread_left(owner, c):
        return pltpu.make_async_remote_copy(
            src_ref=gathered.at[owner, rows_of(c)],
            dst_ref=gathered.at[owner, rows_of(c)],
            send_sem=back_sent.at[owner, c],
            recv_sem=all_got.at[owner, c],
            device_id={"mp": lax.rem(me + last, size)},
            device_id_type=MESH,
        )

    def forward(distance, c):
        @pl.when(me >= distance)
        def _():
            spread_right(me - distance, c).wait_recv()

            @pl.when(me < last)
            def _():
                spread_right(me - distance, c).start()

        @pl.when(me + distance <= last)
        def _():
            spread_left(me + distance, c).wait_recv()

            @pl.when(me > 0)
            def _():
                spread_left(me + distance, c).start()

    def add_into(held, target, c):
        def run(rows):
            held[target, rows, :] = (
                held[target, rows, :].astype(jnp.float32)
                + part[target, rows, :].astype(jnp.float32)
            ).astype(jnp.bfloat16)

        row_loop(c * piece, piece, 16, run)

    def relay(c):
        for far in range(size - 1):
            target = last - far

            @pl.when(me == 0)
            def _():
                to_right(part, target, c).start()

            @pl.when((me > 0) & (me < target))
            def _():
                to_right(from_left, target, c).wait_recv()
                add_into(from_left, target, c)
                to_right(from_left, target, c).start()

            @pl.when(me == last)
            def _():
                to_left(part, far, c).start()

            @pl.when((me < last) & (me > far))
            def _():
                to_left(from_right, far, c).wait_recv()
                add_into(from_right, far, c)
                to_left(from_right, far, c).start()

    def close(c):
        @pl.when(me > 0)
        def _():
            to_right(from_left, me, c).wait_recv()

        @pl.when(me < last)
        def _():
            to_left(from_right, me, c).wait_recv()

        def run(rows):
            total = part[me, rows, :].astype(jnp.float32)
            total = total + from_left[me, rows, :].astype(jnp.float32)
            total = total + from_right[me, rows, :].astype(jnp.float32)
            if spread:
                gathered[me, rows, :] = finish(total, rows, inputs, outputs)
            else:
                gathered[rows, :] = total

        row_loop(c * piece, piece, 16, run)
        if spread:

            @pl.when(me < last)
            def _():
                spread_right(me, c).start()

            @pl.when(me > 0)
            def _():
                spread_left(me, c).start()


    def clear(held, slot):
        def run(rows):
            held[slot, rows, :] = jnp.zeros((16, held.shape[2]), jnp.bfloat16)

        row_loop(0, rows_here, 16, run)

    @pl.when(me == 0)
    def _():
        clear(from_left, 0)

    @pl.when(me == last)
    def _():
        clear(from_right, last)

    for out in outputs[1:]:
        out[...] = jnp.zeros_like(out)
    relay(0)

    def step(c, carry):
        relay(c + 1)
        close(c)
        if spread:
            for distance in range(1, last):

                @pl.when(c >= distance)
                def _(distance=distance):
                    forward(distance, c - distance)

        return carry

    lax.fori_loop(0, PIECES - 1, step, 0)
    close(PIECES - 1)
    if spread:
        for late in range(PIECES - 1, PIECES + last - 1):
            for distance in range(1, last):
                if late - distance < PIECES:
                    forward(distance, late - distance)

    def drain(c, carry):
        if spread:

            @pl.when(me == last)
            def _():
                spread_right(0, c).wait_recv()

            @pl.when(me == 0)
            def _():
                spread_left(last, c).wait_recv()

            for owner in range(size):

                @pl.when((owner <= me) & (me < last))
                def _(owner=owner):
                    spread_right(owner, c).wait_send()

                @pl.when((owner >= me) & (me > 0))
                def _(owner=owner):
                    spread_left(owner, c).wait_send()

        for target in range(1, size):

            @pl.when(me < target)
            def _():
                to_right(from_left, target, c).wait_send()

        for target in range(size - 1):

            @pl.when(me > target)
            def _():
                to_left(from_right, target, c).wait_send()

        return carry

    lax.fori_loop(0, PIECES, drain, 0)


def exchange(finish, partial, inputs, outputs, number):
    size = lax.axis_size("mp")
    part = partial.reshape(size, partial.shape[0] // size, D)
    vmem = pl.BlockSpec(memory_space=pltpu.VMEM)
    got = pl.pallas_call(
        functools.partial(exchange_kernel, size, finish, len(inputs), True),
        out_shape=[jax.ShapeDtypeStruct(part.shape, jnp.bfloat16), *outputs],
        in_specs=[vmem] * (1 + len(inputs)),
        out_specs=[vmem] * (1 + len(outputs)),
        scratch_shapes=[pltpu.VMEM(part.shape, jnp.bfloat16)] * 2
        + [pltpu.SemaphoreType.DMA((size, PIECES))] * 7,
        compiler_params=pltpu.CompilerParams(
            collective_id=number, has_side_effects=True, vmem_limit_bytes=48 << 20
        ),
        cost_estimate=pl.CostEstimate(
            flops=30 * part.size, bytes_accessed=100 * part.size, transcendentals=0
        ),
    )(part, *inputs)
    return got[0].reshape(partial.shape), *got[1:]


def reduce_rows(partial, number):
    size = lax.axis_size("mp")
    part = partial.reshape(size, partial.shape[0] // size, D)
    vmem = pl.BlockSpec(memory_space=pltpu.VMEM)
    return pl.pallas_call(
        functools.partial(exchange_kernel, size, None, 0, False),
        out_shape=jax.ShapeDtypeStruct(part.shape[1:], jnp.float32),
        in_specs=[vmem],
        out_specs=vmem,
        scratch_shapes=[pltpu.VMEM(part.shape, jnp.bfloat16)] * 2
        + [pltpu.SemaphoreType.DMA((size, PIECES))] * 7,
        compiler_params=pltpu.CompilerParams(
            collective_id=number, has_side_effects=True, vmem_limit_bytes=48 << 20
        ),
        cost_estimate=pl.CostEstimate(
            flops=30 * part.size, bytes_accessed=100 * part.size, transcendentals=0
        ),
    )(part)


def lane_mean(values):
    return jnp.sum(values, -1, keepdims=True) * (1.0 / values.shape[-1])


def finish_forward(total, rows, inputs, outputs):
    tokens, scale, gain, bias = inputs
    outputs[0][rows, :] = total
    mid = tokens[rows, :].astype(jnp.float32) + scale[rows, :] * total
    center = mid - lane_mean(mid)
    unit = center * lax.rsqrt(lane_mean(center * center) + epsilon)
    return (unit * gain[...] + bias[...]).astype(jnp.bfloat16)


def finish_backward(total, rows, inputs, outputs):
    tokens, scale, gain, branch, cotangent = inputs
    mid = tokens[rows, :].astype(jnp.float32) + scale[rows, :] * branch[rows, :]
    center = mid - lane_mean(mid)
    inv_std = lax.rsqrt(lane_mean(center * center) + epsilon)
    unit = center * inv_std
    outputs[1][0:1, :] += jnp.sum(total * unit, 0, keepdims=True)
    outputs[1][1:2, :] += jnp.sum(total, 0, keepdims=True)
    scaled = total * gain[...]
    inner = scaled - lane_mean(scaled) - unit * lane_mean(scaled * unit)
    mid_grad = cotangent[rows, :].astype(jnp.float32) + inv_std * inner
    outputs[0][rows, :] = mid_grad
    return (scale[rows, :] * mid_grad).astype(jnp.bfloat16)


def scatter_groups(values, dim):
    return lax.psum_scatter(values, "dp", scatter_dimension=dim, tiled=True)


def sum_over(values, axis_name):
    size = lax.axis_size(axis_name)
    for bit in range(size.bit_length() - 1):
        pairs = [(one, one ^ (1 << bit)) for one in range(size)]
        values = values + lax.ppermute(values, axis_name, pairs)
    return values


def local(
    tokens,
    cotangent,
    ln1_gain,
    ln1_bias,
    w_qkv,
    w_out,
    ln2_gain,
    ln2_bias,
    w_up,
    w_down,
    w_router,
    seq_first,
    head_width,
    ffn_width,
):
    shard_count = lax.axis_size("mp")
    mp_index = lax.axis_index("mp")
    tok_dev = tokens.shape[0]
    group_rows = tok_dev * shard_count
    local_dim = w_qkv.shape[2]
    heads_here = local_dim // HEAD_DIM
    split_at = seq_first[0]
    row_ids = jnp.arange(group_rows, dtype=jnp.int32)
    row_slot = (row_ids >= split_at).astype(jnp.int32)
    positions = (row_ids - row_slot * split_at).astype(jnp.float32)
    slot_hot = (row_slot[None, :] == jnp.arange(2, dtype=jnp.int32)[:, None]).astype(jnp.float32)
    counts = jnp.maximum(jnp.sum(slot_hot, 1), 1.0)
    own_rows = mp_index * tok_dev + jnp.arange(tok_dev, dtype=jnp.int32)
    own_slot = (own_rows >= split_at).astype(jnp.int32)
    own_hot = (own_slot[:, None] == jnp.arange(2, dtype=jnp.int32)[None, :]).astype(jnp.float32)
    head_on = (mp_index < jnp.where(row_slot == 1, head_width[1], head_width[0])).astype(
        jnp.float32
    )
    ffn_on = (mp_index < jnp.where(row_slot == 1, ffn_width[1], ffn_width[0])).astype(jnp.float32)
    x_rows = tokens.astype(jnp.float32)
    normed1, unit1, inv_std1 = norm_rows(x_rows, ln1_gain, ln1_bias)
    h_one = normed1.astype(jnp.bfloat16)
    h_one_all = lax.all_gather(h_one, "mp", axis=0, tiled=True)
    h_one_all, late_cotangent = lax.optimization_barrier((h_one_all, cotangent))
    cotangent_all = lax.all_gather(late_cotangent, "mp", axis=0, tiled=True)
    slot_means = (
        jnp.dot(slot_hot.astype(jnp.bfloat16), h_one_all, preferred_element_type=jnp.float32)
        / counts[:, None]
    )
    logits = jnp.dot(slot_means, w_router, precision=lax.Precision.HIGHEST)
    levels = jnp.arange(shard_count, dtype=jnp.int32)
    pick_head = (levels[None, :] == head_width[:, None] - 1).astype(jnp.float32)
    pick_ffn = (levels[None, :] == ffn_width[:, None] - 1).astype(jnp.float32)
    prob_head = jax.nn.softmax(logits[:, :shard_count], -1)
    prob_ffn = jax.nn.softmax(logits[:, shard_count:], -1)
    scale_head = shard_count * jnp.sum(prob_head * pick_head, 1)
    scale_ffn = shard_count * jnp.sum(prob_ffn * pick_ffn, 1)
    own_scale_head = jnp.where(own_slot == 1, scale_head[1], scale_head[0])[:, None]
    own_scale_ffn = jnp.where(own_slot == 1, scale_ffn[1], scale_ffn[0])[:, None]
    w_qkv_flat = w_qkv.reshape(D, 3 * local_dim)
    qkv_rows = jnp.dot(h_one_all, w_qkv_flat, preferred_element_type=jnp.float32).reshape(
        group_rows, 3, heads_here, HEAD_DIM
    )
    cosine, sine_rows = rotary_tables(positions, HEAD_DIM)
    cosine_b = cosine[:, None, :]
    sine_b = sine_rows[:, None, :]
    query = rotate(qkv_rows[:, 0], cosine_b, sine_b).astype(jnp.bfloat16)
    key_rows = rotate(qkv_rows[:, 1], cosine_b, sine_b).astype(jnp.bfloat16)
    value = qkv_rows[:, 2].astype(jnp.bfloat16)
    inv_root = 1.0 / math.sqrt(HEAD_DIM)
    row_block = min(512, group_rows)

    def scores_block(offset):
        stop = offset + row_block
        query_blk = query[offset : offset + row_block]
        raw_scores = (
            jnp.einsum("thd,shd->hts", query_blk, key_rows[:stop], preferred_element_type=jnp.float32)
            * inv_root
        )
        allowed = (row_slot[offset:stop, None] == row_slot[None, :stop]) & (
            row_ids[None, :stop] <= row_ids[offset:stop, None]
        )
        return jnp.where(allowed[None], raw_scores, masked_score)

    out_list = []
    lse_list = []
    for offset in range(0, group_rows, row_block):
        block_scores = scores_block(offset)
        row_top = jnp.max(block_scores, -1, keepdims=True)
        exp_scores = jnp.exp(block_scores - row_top)
        row_total = jnp.sum(exp_scores, -1, keepdims=True)
        prob_rows = exp_scores / row_total
        lse_list.append(row_top + jnp.log(row_total))
        out_list.append(
            jnp.einsum(
                "hts,shd->thd",
                prob_rows.astype(jnp.bfloat16),
                value[: offset + row_block],
                preferred_element_type=jnp.float32,
            )
        )
    heads_out = jnp.concatenate(out_list, 0)
    attn_mixed = (
        (heads_out * head_on[:, None, None]).astype(jnp.bfloat16).reshape(group_rows, local_dim)
    )
    attn_sent = jnp.dot(attn_mixed, w_out, preferred_element_type=jnp.float32).astype(jnp.bfloat16)
    h_two_all, attn_branch = exchange(
        finish_forward,
        attn_sent,
        (tokens, own_scale_head, ln2_gain[None], ln2_bias[None]),
        (jax.ShapeDtypeStruct((tok_dev, D), jnp.float32),),
        0,
    )
    up_proj = jnp.dot(h_two_all, w_up, preferred_element_type=jnp.float32)
    relu_rows = jnp.maximum(up_proj, 0.0)
    hidden = (relu_rows * relu_rows * ffn_on[:, None]).astype(jnp.bfloat16)
    row_scale_ffn = jnp.where(row_slot == 1, scale_ffn[1], scale_ffn[0])[:, None]
    ffn_grad_all = (row_scale_ffn * cotangent_all.astype(jnp.float32)).astype(jnp.bfloat16)
    hidden_grad = jnp.dot(ffn_grad_all, w_down.T, preferred_element_type=jnp.float32).astype(
        jnp.bfloat16
    )
    grad_up = (hidden_grad.astype(jnp.float32) * (2.0 * relu_rows * ffn_on[:, None])).astype(
        jnp.bfloat16
    )
    normed2_sent = jnp.dot(grad_up, w_up.T, preferred_element_type=jnp.float32).astype(
        jnp.bfloat16
    )
    down_full = jnp.dot(hidden.T, ffn_grad_all, preferred_element_type=jnp.float32).astype(
        jnp.bfloat16
    )
    up_full = jnp.dot(h_two_all.T, grad_up, preferred_element_type=jnp.float32).astype(
        jnp.bfloat16
    )
    down_part = scatter_groups(down_full, 1)
    up_part = scatter_groups(up_full, 0)
    normed2_sent, _, _ = lax.optimization_barrier((normed2_sent, down_full, up_full))
    attn_grad_all, mid_grad, sums2 = exchange(
        finish_backward,
        normed2_sent,
        (tokens, own_scale_head, ln2_gain[None], attn_branch, cotangent),
        (
            jax.ShapeDtypeStruct((tok_dev, D), jnp.float32),
            jax.ShapeDtypeStruct((8, D), jnp.float32),
        ),
        1,
    )
    hidden_late, attn_grad_all = lax.optimization_barrier((hidden, attn_grad_all))
    ffn_sent = jnp.dot(hidden_late, w_down, preferred_element_type=jnp.float32).astype(
        jnp.bfloat16
    )
    attn_grad_all, ffn_sent, down_part, up_part = lax.optimization_barrier(
        (attn_grad_all, ffn_sent, down_part, up_part)
    )
    ffn_branch = lax.psum_scatter(ffn_sent, "mp", scatter_dimension=0, tiled=True)
    mixed_grad = (
        jnp.dot(attn_grad_all, w_out.T, preferred_element_type=jnp.float32)
        .astype(jnp.bfloat16)
        .reshape(group_rows, heads_here, HEAD_DIM)
    )
    mixed_grad = mixed_grad * head_on.astype(jnp.bfloat16)[:, None, None]
    key_grad = 0.0
    value_grad = 0.0

    def at_front(values):
        return jnp.pad(values, ((0, group_rows - values.shape[0]), (0, 0), (0, 0)))

    query_grads = []
    for block_num, offset in enumerate(range(0, group_rows, row_block)):
        block_scores = scores_block(offset)
        prob_rows = jnp.exp(block_scores - lse_list[block_num])
        stop = offset + row_block
        grad_blk = mixed_grad[offset:stop]
        prob_grad = jnp.einsum("thd,shd->hts", grad_blk, value[:stop], preferred_element_type=jnp.float32)
        delta = jnp.sum(prob_rows * prob_grad, -1, keepdims=True)
        score_grad = (prob_rows * (prob_grad - delta)).astype(jnp.bfloat16)
        query_grads.append(
            jnp.einsum("hts,shd->thd", score_grad, key_rows[:stop], preferred_element_type=jnp.float32)
            * inv_root
        )
        key_grad = (
            key_grad
            + at_front(
                jnp.einsum(
                    "hts,thd->shd",
                    score_grad,
                    query[offset:stop],
                    preferred_element_type=jnp.float32,
                )
            )
            * inv_root
        )
        value_grad = value_grad + at_front(
            jnp.einsum(
                "hts,thd->shd",
                prob_rows.astype(jnp.bfloat16),
                grad_blk,
                preferred_element_type=jnp.float32,
            )
        )
    query_grad = jnp.concatenate(query_grads, 0)
    qkv_grad = jnp.stack(
        [
            rotate_back(query_grad, cosine_b, sine_b),
            rotate_back(key_grad, cosine_b, sine_b),
            value_grad,
        ],
        1,
    )
    qkv_grad = qkv_grad.astype(jnp.bfloat16).reshape(group_rows, 3 * local_dim)
    normed1_sent = jnp.dot(qkv_grad, w_qkv_flat.T, preferred_element_type=jnp.float32).astype(
        jnp.bfloat16
    )
    qkv_late, mixed_late, _ = lax.optimization_barrier((qkv_grad, attn_mixed, normed1_sent))
    qkv_full = (
        jnp.dot(h_one_all.T, qkv_late, preferred_element_type=jnp.float32)
        .astype(jnp.bfloat16)
    )
    out_full = jnp.dot(mixed_late.T, attn_grad_all, preferred_element_type=jnp.float32).astype(
        jnp.bfloat16
    )
    normed1_sent, _, _ = lax.optimization_barrier((normed1_sent, qkv_full, out_full))
    normed1_grad = reduce_rows(normed1_sent, 2)
    ffn_branch = ffn_branch.astype(jnp.float32)
    qkv_part = scatter_groups(qkv_full, 0)
    out_part = scatter_groups(out_full, 1)
    mid_rows = x_rows + own_scale_head * attn_branch
    block_out = (mid_rows + own_scale_ffn * ffn_branch).astype(jnp.bfloat16)
    part_head = jnp.sum(own_hot * jnp.sum(mid_grad * attn_branch, 1, keepdims=True), 0)
    part_ffn = jnp.sum(
        own_hot * jnp.sum(cotangent.astype(jnp.float32) * ffn_branch, 1, keepdims=True), 0
    )
    scale_grads = sum_over(jnp.stack([part_head, part_ffn]), "mp")
    logit_head_grad = (scale_grads[0] * scale_head)[:, None] * (pick_head - prob_head)
    logit_ffn_grad = (scale_grads[1] * scale_ffn)[:, None] * (pick_ffn - prob_ffn)
    logit_grad = jnp.concatenate([logit_head_grad, logit_ffn_grad], 1)
    router_part = jnp.dot(logit_grad.T, slot_means, precision=lax.Precision.HIGHEST) / shard_count
    mean_grad = jnp.dot(logit_grad, w_router.T, precision=lax.Precision.HIGHEST) / counts[:, None]
    normed1_grad = normed1_grad + jnp.dot(own_hot, mean_grad, precision=lax.Precision.HIGHEST)
    back_one, gain1_grad, bias1_grad = norm_back(normed1_grad, unit1, inv_std1, ln1_gain)
    input_grad = (mid_grad + back_one).astype(jnp.bfloat16)
    packed = jnp.concatenate([gain1_grad[None], bias1_grad[None], sums2[:2], router_part], 0)
    packed = sum_over(sum_over(packed, "mp"), "dp")
    return (
        block_out,
        input_grad,
        packed[0],
        packed[1],
        qkv_part.astype(jnp.float32).reshape(-1, 3, local_dim),
        out_part.astype(jnp.float32),
        packed[2],
        packed[3],
        up_part.astype(jnp.float32),
        down_part.astype(jnp.float32),
        packed[4:].T,
    )


def solution(mesh):
    placed = (
        P(("dp", "mp"), None),
        P(("dp", "mp"), None),
        P(),
        P(),
        P(None, None, "mp"),
        P("mp", None),
        P(),
        P(),
        P(None, "mp"),
        P("mp", None),
        P(),
        P("dp"),
        P("dp"),
        P("dp"),
    )
    return jax.shard_map(
        local,
        mesh=mesh,
        in_specs=placed,
        out_specs=(
            P(("dp", "mp"), None),
            P(("dp", "mp"), None),
            P(),
            P(),
            P("dp", None, "mp"),
            P("mp", "dp"),
            P(),
            P(),
            P("dp", "mp"),
            P("mp", "dp"),
            P(),
        ),
        check_vma=False,
    )
```
